512 devices in a mesh: seq: 64 (over z_hi, y, x, core), head: 8 (over z_lo).
Axes of the slice: x: 4, y: 4, z: 16 (z_hi: 2, z_lo: 8; z = z_hi * 8 + z_lo), core: 2. Of those that a mesh axis runs over, the one named last changes fastest.
Arguments:
- queries: bfloat16 [49152, 128], P('seq'), may hold values from -6 to 6
- keys: bfloat16 [49152, 128], P('seq'), may hold values from -0.023925781 to 0.023925781
- values: bfloat16 [49152, 8192], P('seq', 'head'), may hold values from -6 to 6
- log_decay: float32 [128, 49152], P('head', 'seq'), may hold values from -0.8 to 0
- level_weight: bfloat16 [7, 128, 49152], P(None, 'head', 'seq'), may hold values from 0.099609375 to 1
- skip: float32 [128], P('head'), may hold values from 0.4 to 4.5
- norm_gain: bfloat16 [8192], P('head'), may hold values from 0.25 to 1.75
Outputs:
- normed: bfloat16 [49152, 8192], P('seq', 'head')
The draws below stay inside these ranges and needn't reach their ends.
All inputs are finite; a program needn't handle non-finite values.
Results may differ from the reference program's by a relative error of at most 0.007.
Values sent between devices are 32-bit elements; how exact they have to be, the bound alone decides.
A program may use at most 128 MiB of HBM per device.

```python
import jax
import jax.numpy as jnp
from jax import lax

HEAD_COUNT = 128
HEAD_DIM = 64
STATE = 128
TOK_DEV = 768
TOKEN_COUNT = 49152
LEVELS = 6
N_SEQ = 64


def draw_log_decay(key, part):
    partition_random_key = jax.random.split(jax.random.fold_in(key, 11), 7)
    slow_share = 0.5
    slow_heads = jax.random.uniform(partition_random_key[0], (HEAD_COUNT,), jnp.float32) < slow_share
    fast_rate = jnp.exp(jax.random.uniform(partition_random_key[1], (HEAD_COUNT,), jnp.float32, jnp.log(1.0 / 50.0), jnp.log(1.0 / 30.0)))
    slow_rate = jnp.exp(jax.random.uniform(partition_random_key[2], (HEAD_COUNT,), jnp.float32, jnp.log(0.02), jnp.log(0.3))) / TOKEN_COUNT
    baseline_decay_rate = jnp.where(slow_heads, slow_rate, fast_rate)[:, None]
    block_multiplier = jax.random.uniform(partition_random_key[3], (HEAD_COUNT, TOKEN_COUNT // TOK_DEV), jnp.float32, 0.5, 1.5)
    block_multiplier = jnp.repeat(block_multiplier, TOK_DEV, axis=1)
    jitter_strength = jax.random.uniform(partition_random_key[4], (HEAD_COUNT, TOKEN_COUNT), jnp.float32, 0.5, 2.0)
    spike_positions = jax.random.randint(partition_random_key[5], (2,), 0, TOKEN_COUNT)
    position_list = jnp.arange(TOKEN_COUNT)
    spike_match = jnp.any(position_list[:, None] == spike_positions[None, :], axis=1)
    spike_penalty = jax.random.uniform(partition_random_key[6], (HEAD_COUNT,), jnp.float32, 0.2, 0.5)
    spike_component = jnp.where(spike_match[None, :], jnp.log(1.0 - spike_penalty)[:, None], 0.0)
    return (-baseline_decay_rate * block_multiplier * jitter_strength + spike_component).astype(jnp.float32)


def draw_skip(key, part):
    head_pos = jnp.arange(HEAD_COUNT, dtype=jnp.float32) / (HEAD_COUNT - 1)
    rough = jax.random.uniform(jax.random.fold_in(key, 29), (HEAD_COUNT,), jnp.float32, 0.5, 1.5)
    return ((1.0 + 2.0 * head_pos) * rough).astype(jnp.float32)


def levels(stream_key, dims, pieces, low, top_value):
    def one(axis_at, blocks):
        heights = jax.random.uniform(jax.random.fold_in(jax.random.fold_in(stream_key, 6), axis_at), (blocks,), jnp.float32, low / len(pieces), top_value / len(pieces))
        return jnp.repeat(jnp.exp(heights), dims[axis_at] // blocks).reshape((-1,) + (1,) * (len(dims) - axis_at - 1))

    gain = one(*pieces[0])
    for cut in pieces[1:]:
        gain = gain * one(*cut)
    return gain


def scatter_about(own_key, shape, deviation, limit, cuts=(), held_as=jnp.bfloat16):
    values = jax.random.normal(own_key, shape, jnp.float32) * deviation
    if len(cuts) > 0:
        values = levels(own_key, shape, cuts, -0.22, 0.18) * values
    return jnp.clip(values, min=-limit, max=limit).astype(held_as)


def setup_inputs(seed: int = 0) -> dict:
    arg_keys = jax.random.split(jax.random.key(seed), 8)
    queries = scatter_about(arg_keys[0], (TOKEN_COUNT, STATE), 1.0, 6.0, ((0, 64),))
    keys = scatter_about(arg_keys[1], (TOKEN_COUNT, STATE), 0.004, 0.023925781, ((0, 64),))
    values = scatter_about(arg_keys[2], (TOKEN_COUNT, HEAD_COUNT * HEAD_DIM), 1.0, 6.0, ((0, 64), (1, 8)))
    log_decay = draw_log_decay(jax.random.fold_in(arg_keys[7], 71), 0)
    level_weight = jnp.clip(0.099609375 + 0.9003906 * jax.random.uniform(arg_keys[4], (LEVELS + 1, HEAD_COUNT, TOKEN_COUNT), jnp.float32) ** levels(arg_keys[4], (LEVELS + 1, HEAD_COUNT, TOKEN_COUNT), ((1, 8), (2, 64)), -0.2, 0.2), 0.099609375, 1.0).astype(jnp.bfloat16)
    skip = draw_skip(jax.random.fold_in(arg_keys[7], 71), 0)
    norm_gain = jnp.clip(1.0 + 0.15 * jax.random.normal(arg_keys[6], (HEAD_COUNT * HEAD_DIM,), jnp.float32), 0.25, 1.75).astype(jnp.bfloat16)
    return {"queries": queries, "keys": keys, "values": values, "log_decay": log_decay, "level_weight": level_weight, "skip": skip, "norm_gain": norm_gain}


def reference(queries, keys, values, log_decay, level_weight, skip, norm_gain):
    blocks = N_SEQ
    span = TOK_DEV
    query_blk = queries.astype(jnp.float32).reshape(blocks, span, STATE)
    key_blk = keys.astype(jnp.float32).reshape(blocks, span, STATE)
    scores = jnp.einsum('dtn,dsn->dts', query_blk, key_blk)
    position = jnp.arange(span, dtype=jnp.int32)
    causal = position[:, None] >= position[None, :]
    head_vals = values.reshape(TOKEN_COUNT, HEAD_COUNT, HEAD_DIM).transpose(1, 0, 2)
    weights_all = level_weight.transpose(1, 0, 2)
    block_ids = jnp.arange(blocks, dtype=jnp.int32)

    def one_head(inputs):
        decay, head_in, lam, skip_one = inputs
        cum_decay = jnp.cumsum(decay.reshape(blocks, span), axis=1)
        vals_f32 = head_in.astype(jnp.float32).reshape(blocks, span, HEAD_DIM)
        lam_f32 = lam.astype(jnp.float32).reshape(LEVELS + 1, blocks, span)
        spread_in = jnp.where(causal[None], cum_decay[:, :, None] - cum_decay[:, None, :], jnp.float32(0.0))
        mixing = (jnp.where(causal[None], jnp.exp(spread_in), jnp.float32(0.0)) * scores).astype(jnp.bfloat16)
        mixing = lax.optimization_barrier(mixing).astype(jnp.float32)
        inner = jnp.einsum('dts,dsp->dtp', mixing, vals_f32)
        tail = jnp.exp(cum_decay[:, -1:] - cum_decay)
        scaled_keys = (key_blk * tail[:, :, None]).astype(jnp.bfloat16)
        scaled_keys = lax.optimization_barrier(scaled_keys).astype(jnp.float32)
        states = jnp.einsum('dsn,dsp->dnp', scaled_keys, vals_f32)
        result = lam_f32[0][:, :, None] * inner + skip_one * vals_f32
        prefix = jnp.concatenate([jnp.zeros((1,), jnp.float32), jnp.cumsum(cum_decay[:, -1])])
        for level_no in range(LEVELS):
            stride = 2 ** level_no
            upper = (block_ids - block_ids % stride).astype(jnp.int32)
            lower = (upper - stride).astype(jnp.int32)
            present = block_ids // stride % 2 == 1
            inside = (block_ids[None, :] >= lower[:, None]) & (block_ids[None, :] < upper[:, None]) & present[:, None]
            spread = jnp.where(inside, prefix[upper][:, None] - prefix[block_ids + 1][None, :], jnp.float32(0.0))
            mixer = jnp.where(inside, jnp.exp(spread), jnp.float32(0.0))
            bucket = jnp.einsum('de,enp->dnp', mixer, states, precision=lax.Precision.HIGHEST)
            gap = prefix[block_ids] - prefix[upper]
            present_f = jnp.where(present, jnp.float32(1.0), jnp.float32(0.0))
            coef = lam_f32[level_no + 1] * present_f[:, None] * jnp.exp(cum_decay + gap[:, None])
            cross = jnp.einsum('dtn,dnp->dtp', query_blk, bucket, precision=lax.Precision.HIGHEST)
            result = result + coef[:, :, None] * cross
        return result.reshape(TOKEN_COUNT, HEAD_DIM)
    mixed_out = lax.map(one_head, (log_decay, head_vals, weights_all, skip))
    squares = lax.optimization_barrier(jnp.sum(mixed_out * mixed_out, axis=(0, 2)))
    inv_rms = lax.rsqrt(squares / (HEAD_COUNT * HEAD_DIM) + 1e-05)
    scaled_out = mixed_out * inv_rms[None, :, None]
    result_all = scaled_out.transpose(1, 0, 2).reshape(TOKEN_COUNT, HEAD_COUNT * HEAD_DIM) * norm_gain.astype(jnp.float32)
    return result_all.astype(jnp.bfloat16)
```

```python
import jax
import jax.numpy as jnp
from jax import lax
from jax.experimental import pallas as pl
from jax.experimental.pallas import tpu as pltpu
from jax.sharding import PartitionSpec as P

F32 = jnp.float32
BF16 = jnp.bfloat16
NT = (((1,), (1,)), ((), ()))

TOK = 768
CH = 128
NC = TOK // CH
HEADS = 16
DIM = 64
STATE = 128
ROWS = HEADS * DIM
HALF = ROWS // 2
PLANE = 32
CHIPS = 16
SLICE = HALF // CHIPS
LEVELS = 6
GROUP = 8
CHANNELS = 8192


def rows_of(start, size):
    return pl.ds(pl.multiple_of(start, SLICE), size)


def kernel(
    q_ref, k_ref, v_ref, ld_ref, lw_ref, skip_ref, gain_ref, out_ref,
    lc_ref, lct_ref, w0_ref, ci_ref, cum_ref, coef_ref, vt_ref, rb_ref, st_ref, acc_ref,
    tot_ref, tots_ref, gath_ref, node_ref, bucket_ref, zin_ref, bb_ref, sq_ref, sqs_ref,
    tot_ss, tot_rs, p1_ss, p1_rs, l0_ss, l0_rs, p2_ss, p2_rs, z_ss, z_rs, fw_ss, fw_rs, sq_ss, sq_rs,
):
    seq = lax.axis_index("seq")
    head = lax.axis_index("head")
    zhi = seq // PLANE
    me = seq % PLANE
    chip = me // 2
    core = me % 2
    base = zhi * PLANE

    def at(s):
        return {"seq": s, "head": head}

    def remote(src, dst, ss, rs, device):
        return pltpu.make_async_remote_copy(
            src_ref=src, dst_ref=dst, send_sem=ss, recv_sem=rs,
            device_id=device, device_id_type=pl.DeviceIdType.MESH,
        )

    partner = at(base + me + 1 - 2 * core)
    zpeer = at(seq + PLANE - 2 * PLANE * zhi)

    barrier = pltpu.get_barrier_semaphore()

    @pl.loop(1, PLANE)
    def _(r):
        pl.semaphore_signal(
            barrier, inc=1, device_id=at(base + (me + r) % PLANE),
            device_id_type=pl.DeviceIdType.MESH)

    @pl.loop(1, GROUP)
    def _(r):
        pl.semaphore_signal(
            barrier, inc=1, device_id={"seq": seq, "head": (head + r) % GROUP},
            device_id_type=pl.DeviceIdType.MESH)

    @pl.when(zhi == 1)
    def _():
        pl.semaphore_signal(
            barrier, inc=1, device_id=zpeer, device_id_type=pl.DeviceIdType.MESH)

    row = lax.broadcasted_iota(jnp.int32, (CH, CH), 0)
    col = lax.broadcasted_iota(jnp.int32, (CH, CH), 1)
    tri = jnp.where(row <= col, 1.0, 0.0).astype(BF16)
    his, mids, los = [], [], []
    for c in range(NC):
        x = ld_ref[:, c * CH:(c + 1) * CH]
        hi = x.astype(BF16)
        rest = x - hi.astype(F32)
        mid = rest.astype(BF16)
        his.append(hi)
        mids.append(mid)
        los.append((rest - mid.astype(F32)).astype(BF16))
    sums = jnp.dot(jnp.concatenate(his + mids + los, axis=0), tri, preferred_element_type=F32)
    n = HEADS * NC
    total = jnp.zeros((HEADS, CH), F32)
    for c in range(NC):
        a = HEADS * c
        lc = sums[a:a + HEADS] + sums[n + a:n + a + HEADS] + sums[2 * n + a:2 * n + a + HEADS]
        lc_ref[c] = lc
        cum_ref[c] = lc + total
        padded = jnp.concatenate([lc, jnp.zeros((CH - HEADS, CH), F32)], axis=0)
        lct_ref[c] = padded.T
        w0 = lw_ref[0, :, c * CH:(c + 1) * CH].astype(F32)
        w0_ref[c] = w0
        ci_ref[c] = w0 * jnp.exp(lc)
        total = total + jnp.broadcast_to(lc[:, CH - 1:CH], (HEADS, CH))
    tot_ref[...] = total
    tots_ref[me] = total

    st_ref[...] = jnp.zeros((ROWS, STATE), F32)

    @pl.loop(0, NC)
    def _(c):
        lc = lc_ref[c]
        last = jnp.broadcast_to(lc[:, CH - 1:CH], (HEADS, CH))
        fall = jnp.exp(last)
        tail = jnp.exp(last - lc)
        scaled = []
        for j in range(ROWS // CH):
            vt = v_ref[c, :, j * CH:(j + 1) * CH].T
            vt_ref[c, j * CH:(j + 1) * CH, :] = vt
            wide = vt.astype(F32)
            for i in range(2):
                h = 2 * j + i
                scaled.append((wide[i * DIM:(i + 1) * DIM] * tail[h:h + 1]).astype(BF16))
        new = jnp.dot(jnp.concatenate(scaled, axis=0), k_ref[c], preferred_element_type=F32)
        for h in range(HEADS):
            rows = slice(h * DIM, (h + 1) * DIM)
            old = st_ref[rows]
            rb_ref[c, rows] = old.astype(BF16)
            st_ref[rows] = fall[h:h + 1] * old + new[rows]

    pl.semaphore_wait(barrier, PLANE - 1 + GROUP - 1 + 1 - zhi)

    @pl.when(core == 0)
    def _():
        remote(st_ref, bucket_ref.at[0], l0_ss, l0_rs, partner).start()

    @pl.loop(1, PLANE)
    def _(r):
        to = (me + r) % PLANE
        dev = at(base + to)
        remote(tot_ref, tots_ref.at[me], tot_ss, tot_rs, dev).start()
        own = HALF * (to % 2) + SLICE * (to // 2)
        remote(st_ref.at[rows_of(own, SLICE)], gath_ref.at[me], p1_ss, p1_rs, dev).start()

    mine = HALF * core + SLICE * chip
    gath_ref[me] = st_ref[rows_of(mine, SLICE)]

    @pl.loop(0, NC)
    def _(c):
        qc = q_ref[c]
        s = lax.dot_general(k_ref[c], qc, NT, preferred_element_type=F32)
        r0 = lax.broadcasted_iota(jnp.int32, (CH, CH), 0)
        c0 = lax.broadcasted_iota(jnp.int32, (CH, CH), 1)
        s = jnp.where(r0 <= c0, s, 0.0)
        inter = lax.dot_general(rb_ref[c], qc, NT, preferred_element_type=F32)
        for h in range(HEADS):
            rows = slice(h * DIM, (h + 1) * DIM)
            d = jnp.minimum(lc_ref[c, h:h + 1] - lct_ref[c, :, h:h + 1], 0.0)
            mix = (jnp.exp(d) * s).astype(BF16)
            vt = vt_ref[c, rows]
            o = jnp.dot(vt, mix, preferred_element_type=F32)
            acc_ref[c, rows] = (
                w0_ref[c, h:h + 1] * o + ci_ref[c, h:h + 1] * inter[rows]
                + skip_ref[h] * vt.astype(F32))

    remote(tots_ref.at[pl.ds(0, PLANE - 1)], tots_ref.at[pl.ds(0, PLANE - 1)], tot_ss, tot_rs,
           partner).wait_recv()
    remote(gath_ref.at[pl.ds(0, PLANE - 1)], gath_ref.at[pl.ds(0, PLANE - 1)], p1_ss, p1_rs,
           partner).wait_recv()
    hd = 8 * core + chip // 2
    nodes = [gath_ref[i] for i in range(PLANE)]
    weights = [tots_ref[i, pl.ds(hd, 1), :] for i in range(PLANE)]
    slot = 0
    for level in range(1, LEVELS):
        joined = [
            jnp.exp(weights[2 * j + 1]) * nodes[2 * j] + nodes[2 * j + 1]
            for j in range(len(nodes) // 2)
        ]
        weights = [weights[2 * j] + weights[2 * j + 1] for j in range(len(nodes) // 2)]
        nodes = joined
        for j in range(0, len(nodes), 2):
            node_ref[slot] = nodes[j]
            slot += 1
    starts = [0, 0, 8, 12, 14, 15]

    @pl.when(zhi == 0)
    def _():
        remote(node_ref.at[starts[5]], zin_ref, z_ss, z_rs, zpeer).start()

    bits = [core] + [(chip // (1 << b)) % 2 for b in range(4)] + [zhi]

    @pl.loop(1, CHIPS)
    def _(r):
        to = (chip + r) % CHIPS
        dev = at(base + 2 * to + core)
        for level in range(1, 5):
            @pl.when((to // (1 << (level - 1))) % 2 == 1)
            def _():
                remote(
                    node_ref.at[starts[level] + to // (1 << level)],
                    bucket_ref.at[level, rows_of(mine, SLICE)],
                    p2_ss.at[level - 1], p2_rs.at[level - 1], dev).start()

    for level in range(1, 5):
        @pl.when(bits[level] == 1)
        def _():
            bucket_ref[level, rows_of(mine, SLICE)] = node_ref[starts[level] + chip // (1 << level)]

    offs = [jnp.zeros((HEADS, CH), F32) for _ in range(LEVELS)]
    for i in range(PLANE - 1):
        t = tots_ref[i]
        for level in range(1, LEVELS):
            inside = (i < me) & (i >= me - me % (1 << level))
            offs[level] = offs[level] + jnp.where(inside, t, 0.0)
    for level in range(LEVELS):
        for c in range(NC):
            w = lw_ref[level + 1, :, c * CH:(c + 1) * CH].astype(F32)
            coef_ref[level, c] = w * jnp.exp(cum_ref[c] + offs[level])

    def cross(level):
        bb_ref[...] = bucket_ref[level].astype(BF16)

        @pl.loop(0, NC // 2)
        def _(d):
            q2 = q_ref[pl.ds(2 * d, 2)].reshape(2 * CH, STATE)
            o = lax.dot_general(bb_ref[...], q2, NT, preferred_element_type=F32)
            for i in range(2):
                c = 2 * d + i
                for h in range(HEADS):
                    rows = slice(h * DIM, (h + 1) * DIM)
                    acc_ref[c, rows] = (
                        acc_ref[c, rows]
                        + coef_ref[level, c, h:h + 1] * o[rows, i * CH:(i + 1) * CH])

    half = rows_of(HALF * core, HALF)
    other = rows_of(HALF * (1 - core), HALF)
    some = pl.ds(0, (CHIPS - 1) * SLICE)

    @pl.when(core == 1)
    def _():
        remote(st_ref, bucket_ref.at[0], l0_ss, l0_rs, partner).wait_recv()
        cross(0)

    for level in range(1, 5):
        @pl.when(bits[level] == 1)
        def _():
            remote(
                bucket_ref.at[level, some], bucket_ref.at[level, some],
                p2_ss.at[level - 1], p2_rs.at[level - 1], partner).wait_recv()
            remote(
                bucket_ref.at[level, half], bucket_ref.at[level, half],
                fw_ss.at[level - 1], fw_rs.at[level - 1], partner).start()

    @pl.when(zhi == 1)
    def _():
        remote(zin_ref, zin_ref, z_ss, z_rs, zpeer).wait_recv()

        @pl.loop(1, CHIPS)
        def _(r):
            to = (chip + r) % CHIPS
            remote(
                zin_ref, bucket_ref.at[5, rows_of(mine, SLICE)],
                p2_ss.at[4], p2_rs.at[4], at(base + 2 * to + core)).start()
        bucket_ref[5, rows_of(mine, SLICE)] = zin_ref[...]

    for level in range(1, 5):
        @pl.when(bits[level] == 1)
        def _():
            remote(
                bucket_ref.at[level, half], bucket_ref.at[level, other],
                fw_ss.at[level - 1], fw_rs.at[level - 1], partner).wait_recv()
            cross(level)

    @pl.when(zhi == 1)
    def _():
        remote(
            bucket_ref.at[5, some], bucket_ref.at[5, some],
            p2_ss.at[4], p2_rs.at[4], partner).wait_recv()
        remote(
            bucket_ref.at[5, half], bucket_ref.at[5, half],
            fw_ss.at[4], fw_rs.at[4], partner).start()
        remote(
            bucket_ref.at[5, half], bucket_ref.at[5, other],
            fw_ss.at[4], fw_rs.at[4], partner).wait_recv()
        cross(5)

    sq_ref[...] = jnp.zeros((8, CH), F32)
    for c in range(NC):
        y = acc_ref[c]
        sq_ref[c:c + 1] = jnp.sum(y * y, axis=0, keepdims=True)
    sqs_ref[head] = sq_ref[...]

    @pl.loop(1, GROUP)
    def _(r):
        remote(
            sq_ref, sqs_ref.at[head], sq_ss, sq_rs,
            {"seq": seq, "head": (head + r) % GROUP}).start()

    remote(tots_ref.at[pl.ds(0, PLANE - 1)], tots_ref.at[pl.ds(0, PLANE - 1)], tot_ss, tot_rs,
           partner).wait_send()
    remote(gath_ref.at[pl.ds(0, PLANE - 1)], gath_ref.at[pl.ds(0, PLANE - 1)], p1_ss, p1_rs,
           partner).wait_send()

    @pl.when(core == 0)
    def _():
        remote(st_ref, bucket_ref.at[0], l0_ss, l0_rs, partner).wait_send()

    for level in range(1, 5):
        for has in range(2):
            @pl.when(bits[level] == has)
            def _():
                some_sent = pl.ds(0, (CHIPS // 2 - has) * SLICE)
                remote(
                    bucket_ref.at[level, some_sent], bucket_ref.at[level, some_sent],
                    p2_ss.at[level - 1], p2_rs.at[level - 1], partner).wait_send()

        @pl.when(bits[level] == 1)
        def _():
            remote(
                bucket_ref.at[level, half], bucket_ref.at[level, half],
                fw_ss.at[level - 1], fw_rs.at[level - 1], partner).wait_send()

    @pl.when(zhi == 0)
    def _():
        remote(node_ref.at[starts[5]], zin_ref, z_ss, z_rs, zpeer).wait_send()

    @pl.when(zhi == 1)
    def _():
        remote(
            bucket_ref.at[5, some], bucket_ref.at[5, some],
            p2_ss.at[4], p2_rs.at[4], partner).wait_send()
        remote(
            bucket_ref.at[5, half], bucket_ref.at[5, half],
            fw_ss.at[4], fw_rs.at[4], partner).wait_send()

    seven = sqs_ref.at[pl.ds(0, GROUP - 1)]
    remote(seven, seven, sq_ss, sq_rs, partner).wait_recv()
    whole = sqs_ref[0]
    for g in range(1, GROUP):
        whole = whole + sqs_ref[g]
    remote(seven, seven, sq_ss, sq_rs, partner).wait_send()
    sq_ref[...] = lax.rsqrt(whole / CHANNELS + 1e-05)

    @pl.loop(0, NC)
    def _(c):
        inv = sq_ref[pl.ds(c, 1), :]
        for j in range(ROWS // CH):
            cols = slice(j * CH, (j + 1) * CH)
            y = (acc_ref[c, cols] * inv).T
            out_ref[c, :, cols] = (y * gain_ref[:, cols].astype(F32)).astype(BF16)


def shards(queries, keys, values, log_decay, level_weight, skip, norm_gain):
    vmem = pl.BlockSpec(memory_space=pltpu.VMEM)
    dma = pltpu.SemaphoreType.DMA
    out = pl.pallas_call(
        kernel,
        out_shape=jax.ShapeDtypeStruct((NC, CH, ROWS), BF16),
        in_specs=[vmem] * 5 + [pl.BlockSpec(memory_space=pltpu.SMEM), vmem],
        out_specs=vmem,
        scratch_shapes=[
            pltpu.VMEM((NC, HEADS, CH), F32),
            pltpu.VMEM((NC, CH, CH), F32),
            pltpu.VMEM((NC, HEADS, CH), F32),
            pltpu.VMEM((NC, HEADS, CH), F32),
            pltpu.VMEM((NC, HEADS, CH), F32),
            pltpu.VMEM((LEVELS, NC, HEADS, CH), F32),
            pltpu.VMEM((NC, ROWS, CH), BF16),
            pltpu.VMEM((NC, ROWS, STATE), BF16),
            pltpu.VMEM((ROWS, STATE), F32),
            pltpu.VMEM((NC, ROWS, CH), F32),
            pltpu.VMEM((HEADS, CH), F32),
            pltpu.VMEM((PLANE, HEADS, CH), F32),
            pltpu.VMEM((PLANE, SLICE, STATE), F32),
            pltpu.VMEM((CHIPS, SLICE, STATE), F32),
            pltpu.VMEM((LEVELS, ROWS, STATE), F32),
            pltpu.VMEM((SLICE, STATE), F32),
            pltpu.VMEM((ROWS, STATE), BF16),
            pltpu.VMEM((8, CH), F32),
            pltpu.VMEM((GROUP, 8, CH), F32),
            dma, dma, dma, dma, dma, dma, dma((5,)), dma((5,)), dma, dma, dma((5,)), dma((5,)),
            dma, dma,
        ],
        compiler_params=pltpu.CompilerParams(
            collective_id=0, has_side_effects=True, vmem_limit_bytes=50 << 20),
        name="layer",
    )(
        queries.reshape(NC, CH, STATE), keys.reshape(NC, CH, STATE), values.reshape(NC, CH, ROWS),
        log_decay, level_weight, skip, norm_gain.reshape(1, ROWS),
    )
    return out.reshape(TOK, ROWS)


def solution(mesh):
    placed = (
        P("seq", None), P("seq", None), P("seq", "head"), P("head", "seq"),
        P(None, "head", "seq"), P("head"), P("head"),
    )
    return jax.shard_map(
        shards, mesh=mesh, in_specs=placed, out_specs=P("seq", "head"), check_vma=False
    )
```

```python
import jax
import jax.numpy as jnp
from jax import lax
from jax.experimental import pallas as pl
from jax.experimental.pallas import tpu as pltpu
from jax.sharding import PartitionSpec as P

F32 = jnp.float32
BF16 = jnp.bfloat16
NT = (((1,), (1,)), ((), ()))

TOK = 768
CH = 128
NC = TOK // CH
HEADS = 16
HH = HEADS // 2
DIM = 64
STATE = 128
ROWS = HEADS * DIM
HALF = ROWS // 2
PLANE = 32
CHIPS = 16
SLICE = HALF // CHIPS
LEVELS = 6
GROUP = 8
CHANNELS = 8192
STARTS = {2: 0, 3: 4, 4: 6, 5: 7}


def rows_of(start, size):
    return pl.ds(pl.multiple_of(start, SLICE), size)


def kernel(
    q_hbm, k_hbm, v_hbm, ld_hbm, lw_hbm, skip_hbm, gain_hbm, out_ref,
    q_ref, k_ref, v_ref, ld_ref, lw_ref, skip_ref, gain_ref, in_sem,
    lc_ref, lct_ref, w0_ref, ci_ref, cum_ref, coef_ref, vt_ref, rb_ref, st_ref, acc_ref, y_ref,
    comb_ref, pcomb_ref, fall_ref, pair_ref, crow_ref, crows_ref,
    gath_ref, node_ref, bucket_ref, zin_ref, bb_ref, sq_ref, sqs_ref,
    ex_ss, ex_rs, cb_ss, cb_rs, l0_ss, l0_rs, cr_ss, cr_rs, p1_ss, p1_rs, n1_ss, n1_rs,
    p2_ss, p2_rs, z_ss, z_rs, fw_ss, fw_rs, sq_ss, sq_rs,
):
    seq = lax.axis_index("seq")
    head = lax.axis_index("head")
    zhi = seq // PLANE
    me = seq % PLANE
    chip = me // 2
    core = me % 2
    base = zhi * PLANE
    bits = [core] + [(chip // (1 << b)) % 2 for b in range(4)] + [zhi]

    def at(s):
        return {"seq": s, "head": head}

    def same_core(to):
        return at(base + 2 * to + core)

    def remote(src, dst, ss, rs, device):
        return pltpu.make_async_remote_copy(
            src_ref=src, dst_ref=dst, send_sem=ss, recv_sem=rs,
            device_id=device, device_id_type=pl.DeviceIdType.MESH,
        )

    partner = at(base + me + 1 - 2 * core)
    zpeer = at(seq + PLANE - 2 * PLANE * zhi)
    half = rows_of(HALF * core, HALF)
    other = rows_of(HALF * (1 - core), HALF)
    mine = HALF * core + SLICE * chip

    pairs = [(ld_hbm, ld_ref), (k_hbm, k_ref), (lw_hbm, lw_ref), (q_hbm, q_ref),
             (skip_hbm, skip_ref), (gain_hbm, gain_ref)]
    loads = [pltpu.make_async_copy(src, dst, in_sem.at[i]) for i, (src, dst) in enumerate(pairs)]
    loads[0].start()
    for c in range(NC):
        pltpu.make_async_copy(v_hbm.at[c], v_ref.at[c], in_sem.at[6 + c]).start()
    for copy in loads[1:]:
        copy.start()

    barrier = pltpu.get_barrier_semaphore()

    def greet(device):
        pl.semaphore_signal(
            barrier, inc=1, device_id=device, device_id_type=pl.DeviceIdType.MESH)

    @pl.loop(1, CHIPS)
    def _(r):
        greet(same_core((chip + r) % CHIPS))

    @pl.loop(1, GROUP)
    def _(r):
        greet({"seq": seq, "head": (head + r) % GROUP})

    greet(partner)

    @pl.when(zhi == 1)
    def _():
        greet(zpeer)

    loads[0].wait()
    loads[2].wait()
    row = lax.broadcasted_iota(jnp.int32, (CH, CH), 0)
    col = lax.broadcasted_iota(jnp.int32, (CH, CH), 1)
    tri = jnp.where(row <= col, 1.0, 0.0).astype(BF16)
    his, mids, los = [], [], []
    for c in range(NC):
        x = ld_ref[:, c * CH:(c + 1) * CH]
        hi = x.astype(BF16)
        rest = x - hi.astype(F32)
        mid = rest.astype(BF16)
        his.append(hi)
        mids.append(mid)
        los.append((rest - mid.astype(F32)).astype(BF16))
    sums = jnp.dot(jnp.concatenate(his + mids + los, axis=0), tri, preferred_element_type=F32)
    n = HEADS * NC
    total = jnp.zeros((HEADS, CH), F32)
    trow = jnp.zeros((1, CH), F32)
    for c in range(NC):
        a = HEADS * c
        lc = sums[a:a + HEADS] + sums[n + a:n + a + HEADS] + sums[2 * n + a:2 * n + a + HEADS]
        lc_ref[c] = lc
        cum_ref[c] = lc + total
        turned = jnp.concatenate([lc, jnp.zeros((CH - HEADS, CH), F32)], axis=0).T
        lct_ref[c] = turned
        trow = trow + turned[CH - 1:CH]
        w0 = lw_ref[0, :, c * CH:(c + 1) * CH].astype(F32)
        w0_ref[c] = w0
        ci_ref[c] = w0 * jnp.exp(lc)
        total = total + jnp.broadcast_to(lc[:, CH - 1:CH], (HEADS, CH))
    comb_ref[0:HEADS] = total
    comb_ref[HEADS:HEADS + 8] = jnp.broadcast_to(trow, (8, CH))

    st_ref[...] = jnp.zeros((ROWS, STATE), F32)
    loads[1].wait()

    @pl.loop(0, NC)
    def _(c):
        pltpu.make_async_copy(v_hbm.at[c], v_ref.at[c], in_sem.at[6 + c]).wait()
        lc = lc_ref[c]
        last = jnp.broadcast_to(lc[:, CH - 1:CH], (HEADS, CH))
        fall = jnp.exp(last)
        tail = jnp.exp(last - lc)
        scaled = []
        for j in range(ROWS // CH):
            vt = v_ref[c, :, j * CH:(j + 1) * CH].T
            vt_ref[c, j * CH:(j + 1) * CH, :] = vt
            wide = vt.astype(F32)
            for i in range(2):
                h = 2 * j + i
                scaled.append((wide[i * DIM:(i + 1) * DIM] * tail[h:h + 1]).astype(BF16))
        new = jnp.dot(jnp.concatenate(scaled, axis=0), k_ref[c], preferred_element_type=F32)
        for h in range(HEADS):
            rows = slice(h * DIM, (h + 1) * DIM)
            old = st_ref[rows]
            rb_ref[c, rows] = old.astype(BF16)
            st_ref[rows] = fall[h:h + 1] * old + new[rows]

    pl.semaphore_wait(barrier, CHIPS - 1 + GROUP - 1 + 1 + 1 - zhi)

    swap = remote(st_ref.at[other], bucket_ref.at[0, other], ex_ss, ex_rs, partner)
    comb = remote(comb_ref, pcomb_ref, cb_ss, cb_rs, partner)
    zero = remote(st_ref.at[half], bucket_ref.at[0, half], l0_ss, l0_rs, partner)
    swap.start()
    comb.start()

    @pl.when(core == 0)
    def _():
        zero.start()

    for copy in loads[3:]:
        copy.wait()

    def inside(first, last):
        @pl.loop(first, last)
        def _(c):
            qc = q_ref[c]
            s = lax.dot_general(k_ref[c], qc, NT, preferred_element_type=F32)
            r0 = lax.broadcasted_iota(jnp.int32, (CH, CH), 0)
            c0 = lax.broadcasted_iota(jnp.int32, (CH, CH), 1)
            s = jnp.where(r0 <= c0, s, 0.0)
            inter = lax.dot_general(rb_ref[c], qc, NT, preferred_element_type=F32)
            for h in range(HEADS):
                rows = slice(h * DIM, (h + 1) * DIM)
                d = jnp.minimum(lc_ref[c, h:h + 1] - lct_ref[c, :, h:h + 1], 0.0)
                mix = (jnp.exp(d) * s).astype(BF16)
                vt = vt_ref[c, rows]
                o = jnp.dot(vt, mix, preferred_element_type=F32)
                acc_ref[c, rows] = (
                    w0_ref[c, h:h + 1] * o + ci_ref[c, h:h + 1] * inter[rows]
                    + skip_ref[h] * vt.astype(F32))

    inside(0, 2)

    comb.wait_recv()
    remote(st_ref.at[half], bucket_ref.at[0, half], ex_ss, ex_rs, partner).wait_recv()
    late = jnp.where(core == 0, pcomb_ref[0:HEADS], comb_ref[0:HEADS])
    fall_ref[...] = jnp.exp(late)
    for i in range(HH):
        at_head = rows_of(HALF * core + DIM * i, DIM)
        own, got = st_ref[at_head], bucket_ref[0, at_head]
        left = jnp.where(core == 0, own, got)
        right = jnp.where(core == 0, got, own)
        pair_ref[i * DIM:(i + 1) * DIM] = fall_ref[pl.ds(HH * core + i, 1), :] * left + right
    crow = comb_ref[HEADS:HEADS + 1] + pcomb_ref[HEADS:HEADS + 1]
    crow_ref[...] = crow
    crows_ref[chip] = crow

    @pl.loop(1, CHIPS)
    def _(r):
        to = (chip + r) % CHIPS
        remote(pair_ref.at[rows_of(SLICE * to, SLICE)], gath_ref.at[chip], p1_ss, p1_rs,
               same_core(to)).start()
        remote(crow_ref, crows_ref.at[chip], cr_ss, cr_rs, same_core(to)).start()

    first_level = remote(
        pair_ref, bucket_ref.at[1, half], n1_ss, n1_rs, same_core(chip + 1 - 2 * bits[1]))

    @pl.when(bits[1] == 0)
    def _():
        first_level.start()

    gath_ref[chip] = pair_ref[rows_of(SLICE * chip, SLICE)]

    inside(2, NC)

    fifteen = pl.ds(0, CHIPS - 1)
    crs = remote(crows_ref.at[fifteen], crows_ref.at[fifteen], cr_ss, cr_rs, partner)
    p1s = remote(gath_ref.at[fifteen], gath_ref.at[fifteen], p1_ss, p1_rs, partner)
    crs.wait_recv()
    p1s.wait_recv()

    lane = lax.broadcasted_iota(jnp.int32, (1, CH), 1)
    pick = lane == HH * core + chip // 2
    nodes = [gath_ref[i] for i in range(CHIPS)]
    weights = [
        jnp.sum(jnp.where(pick, crows_ref[i], 0.0), axis=1, keepdims=True) for i in range(CHIPS)]
    slot = 0
    for level in range(2, LEVELS):
        count = len(nodes) // 2
        joined = [
            jnp.exp(jnp.broadcast_to(weights[2 * j + 1], (1, CH))) * nodes[2 * j] + nodes[2 * j + 1]
            for j in range(count)
        ]
        weights = [weights[2 * j] + weights[2 * j + 1] for j in range(count)]
        nodes = joined
        for j in range(0, count, 2):
            node_ref[slot] = nodes[j]
            slot += 1

    up = remote(node_ref.at[STARTS[5]], zin_ref, z_ss, z_rs, zpeer)

    @pl.when(zhi == 0)
    def _():
        up.start()

    @pl.loop(1, CHIPS)
    def _(r):
        to = (chip + r) % CHIPS
        for level in range(2, 5):
            @pl.when((to // (1 << (level - 1))) % 2 == 1)
            def _():
                remote(
                    node_ref.at[STARTS[level] + to // (1 << level)],
                    bucket_ref.at[level, rows_of(mine, SLICE)],
                    p2_ss.at[level], p2_rs.at[level], same_core(to)).start()

    for level in range(2, 5):
        @pl.when(bits[level] == 1)
        def _():
            bucket_ref[level, rows_of(mine, SLICE)] = node_ref[STARTS[level] + chip // (1 << level)]

    before = [jnp.zeros((1, CH), F32) for _ in range(LEVELS)]
    for i in range(CHIPS - 1):
        t = crows_ref[i]
        for level in range(2, LEVELS):
            counts = (i < chip) & (i >= chip - chip % (1 << (level - 1)))
            before[level] = before[level] + jnp.where(counts, t, 0.0)
    turned = jnp.concatenate(before + [jnp.zeros((CH - LEVELS, CH), F32)], axis=0).T
    inner = jnp.where(core == 1, pcomb_ref[0:HEADS], 0.0)
    for level in range(LEVELS):
        off = jnp.zeros((HEADS, CH), F32)
        if level > 0:
            off = inner
        if level > 1:
            off = off + jnp.broadcast_to(turned[0:HEADS, level:level + 1], (HEADS, CH))
        for c in range(NC):
            w = lw_ref[level + 1, :, c * CH:(c + 1) * CH].astype(F32)
            coef_ref[level, c] = w * jnp.exp(cum_ref[c] + off)

    def cross(level, side):
        at_half = rows_of(HALF * side, HALF)
        bb_ref[...] = bucket_ref[level, at_half].astype(BF16)

        @pl.loop(0, NC // 2)
        def _(d):
            q2 = q_ref[pl.ds(2 * d, 2)].reshape(2 * CH, STATE)
            o = lax.dot_general(bb_ref[...], q2, NT, preferred_element_type=F32)
            for i in range(2):
                c = 2 * d + i
                for h in range(HH):
                    rows = rows_of(HALF * side + DIM * h, DIM)
                    acc_ref[c, rows] = (
                        acc_ref[c, rows]
                        + coef_ref[level, c, pl.ds(HH * side + h, 1), :]
                        * o[h * DIM:(h + 1) * DIM, i * CH:(i + 1) * CH])

    def forward(level):
        return remote(
            bucket_ref.at[level, half], bucket_ref.at[level, half],
            fw_ss.at[level], fw_rs.at[level], partner)

    def forwarded(level):
        return remote(
            bucket_ref.at[level, other], bucket_ref.at[level, other],
            fw_ss.at[level], fw_rs.at[level], partner)

    some = pl.ds(0, (CHIPS - 1) * SLICE)

    def slices(level):
        part = bucket_ref.at[level, some]
        return remote(part, part, p2_ss.at[level], p2_rs.at[level], partner)

    @pl.when(core == 1)
    def _():
        cross(0, core)
        remote(st_ref.at[other], bucket_ref.at[0, other], l0_ss, l0_rs, partner).wait_recv()
        cross(0, 1 - core)

    @pl.when(bits[1] == 1)
    def _():
        first_level.wait_recv()
        forward(1).start()
        cross(1, core)
        forwarded(1).wait_recv()
        cross(1, 1 - core)

    @pl.when(zhi == 1)
    def _():
        up.wait_recv()

        @pl.loop(1, CHIPS)
        def _(r):
            remote(
                zin_ref, bucket_ref.at[5, rows_of(mine, SLICE)],
                p2_ss.at[5], p2_rs.at[5], same_core((chip + r) % CHIPS)).start()
        bucket_ref[5, rows_of(mine, SLICE)] = zin_ref[...]

    for level in range(2, 5):
        @pl.when(bits[level] == 1)
        def _():
            slices(level).wait_recv()
            forward(level).start()

    for level in range(2, 5):
        @pl.when(bits[level] == 1)
        def _():
            cross(level, core)
            forwarded(level).wait_recv()
            cross(level, 1 - core)

    @pl.when(zhi == 1)
    def _():
        slices(5).wait_recv()
        forward(5).start()

    @pl.when(zhi == 1)
    def _():
        cross(5, core)
        forwarded(5).wait_recv()
        cross(5, 1 - core)

    sq_ref[...] = jnp.zeros((8, CH), F32)
    for c in range(NC):
        y = acc_ref[c]
        sq_ref[c:c + 1] = jnp.sum(y * y, axis=0, keepdims=True)
    sqs_ref[head] = sq_ref[...]

    @pl.loop(1, GROUP)
    def _(r):
        remote(
            sq_ref, sqs_ref.at[head], sq_ss, sq_rs,
            {"seq": seq, "head": (head + r) % GROUP}).start()

    gain = gain_ref[...].reshape(1, ROWS).astype(F32)

    @pl.loop(0, NC)
    def _(c):
        for j in range(ROWS // CH):
            cols = slice(j * CH, (j + 1) * CH)
            y_ref[c, :, cols] = acc_ref[c, cols].T * gain[:, cols]

    swap.wait_send()
    comb.wait_send()
    crs.wait_send()
    p1s.wait_send()

    @pl.when(core == 0)
    def _():
        zero.wait_send()

    @pl.when(bits[1] == 0)
    def _():
        first_level.wait_send()

    @pl.when(bits[1] == 1)
    def _():
        forward(1).wait_send()

    for level in range(2, 5):
        for has in range(2):
            @pl.when(bits[level] == has)
            def _():
                sent = bucket_ref.at[level, pl.ds(0, (CHIPS // 2 - has) * SLICE)]
                remote(sent, sent, p2_ss.at[level], p2_rs.at[level], partner).wait_send()

        @pl.when(bits[level] == 1)
        def _():
            forward(level).wait_send()

    @pl.when(zhi == 0)
    def _():
        up.wait_send()

    @pl.when(zhi == 1)
    def _():
        slices(5).wait_send()
        forward(5).wait_send()

    seven = sqs_ref.at[pl.ds(0, GROUP - 1)]
    remote(seven, seven, sq_ss, sq_rs, partner).wait_recv()
    remote(seven, seven, sq_ss, sq_rs, partner).wait_send()

    whole = sqs_ref[0]
    for g in range(1, GROUP):
        whole = whole + sqs_ref[g]
    inv = lax.rsqrt(whole / CHANNELS + 1e-05)
    turned = jnp.concatenate([inv, jnp.zeros((CH - 8, CH), F32)], axis=0).T
    for c in range(NC):
        out_ref[c] = (y_ref[c] * turned[:, c:c + 1]).astype(BF16)


def shards(queries, keys, values, log_decay, level_weight, skip, norm_gain):
    hbm = pl.BlockSpec(memory_space=pltpu.HBM)
    dma = pltpu.SemaphoreType.DMA

    def stay(x):
        return pltpu.with_memory_space_constraint(x, pltpu.HBM)

    out = pl.pallas_call(
        kernel,
        out_shape=jax.ShapeDtypeStruct((NC, CH, ROWS), BF16),
        in_specs=[hbm] * 7,
        out_specs=pl.BlockSpec(memory_space=pltpu.VMEM),
        scratch_shapes=[
            pltpu.VMEM((NC, CH, STATE), BF16),
            pltpu.VMEM((NC, CH, STATE), BF16),
            pltpu.VMEM((NC, CH, ROWS), BF16),
            pltpu.VMEM((HEADS, TOK), F32),
            pltpu.VMEM((LEVELS + 1, HEADS, TOK), BF16),
            pltpu.SMEM((HEADS,), F32),
            pltpu.VMEM((ROWS,), BF16),
            dma((6 + NC,)),
            pltpu.VMEM((NC, HEADS, CH), F32),
            pltpu.VMEM((NC, CH, CH), F32),
            pltpu.VMEM((NC, HEADS, CH), F32),
            pltpu.VMEM((NC, HEADS, CH), F32),
            pltpu.VMEM((NC, HEADS, CH), F32),
            pltpu.VMEM((LEVELS, NC, HEADS, CH), F32),
            pltpu.VMEM((NC, ROWS, CH), BF16),
            pltpu.VMEM((NC, ROWS, STATE), BF16),
            pltpu.VMEM((ROWS, STATE), F32),
            pltpu.VMEM((NC, ROWS, CH), F32),
            pltpu.VMEM((NC, CH, ROWS), F32),
            pltpu.VMEM((HEADS + 8, CH), F32),
            pltpu.VMEM((HEADS + 8, CH), F32),
            pltpu.VMEM((HEADS, CH), F32),
            pltpu.VMEM((HALF, STATE), F32),
            pltpu.VMEM((1, CH), F32),
            pltpu.VMEM((CHIPS, 1, CH), F32),
            pltpu.VMEM((CHIPS, SLICE, STATE), F32),
            pltpu.VMEM((8, SLICE, STATE), F32),
            pltpu.VMEM((LEVELS, ROWS, STATE), F32),
            pltpu.VMEM((SLICE, STATE), F32),
            pltpu.VMEM((HALF, STATE), BF16),
            pltpu.VMEM((8, CH), F32),
            pltpu.VMEM((GROUP, 8, CH), F32),
            dma, dma, dma, dma, dma, dma, dma, dma, dma, dma, dma, dma,
            dma((LEVELS,)), dma((LEVELS,)), dma, dma, dma((LEVELS,)), dma((LEVELS,)), dma, dma,
        ],
        compiler_params=pltpu.CompilerParams(
            collective_id=0, has_side_effects=True, vmem_limit_bytes=50 << 20),
        name="layer",
    )(
        stay(queries.reshape(NC, CH, STATE)), stay(keys.reshape(NC, CH, STATE)),
        stay(values.reshape(NC, CH, ROWS)), stay(log_decay), stay(level_weight), stay(skip),
        stay(norm_gain),
    )
    return out.reshape(TOK, ROWS)


def solution(mesh):
    placed = (
        P("seq", None), P("seq", None), P("seq", "head"), P("head", "seq"),
        P(None, "head", "seq"), P("head"), P("head"),
    )
    return jax.shard_map(
        shards, mesh=mesh, in_specs=placed, out_specs=P("seq", "head"), check_vma=False
    )
```

```python
import jax
import jax.numpy as jnp
from jax import lax
from jax.experimental import pallas as pl
from jax.experimental.pallas import tpu as pltpu
from jax.sharding import PartitionSpec as P

F32 = jnp.float32
BF16 = jnp.bfloat16
NT = (((1,), (1,)), ((), ()))

TOK = 768
CH = 128
NC = TOK // CH
HEADS = 16
HH = HEADS // 2
DIM = 64
STATE = 128
ROWS = HEADS * DIM
HALF = ROWS // 2
PLANE = 32
CHIPS = 16
SLICE = HALF // CHIPS
LEVELS = 6
GROUP = 8
CHANNELS = 8192
STARTS = {2: 0, 3: 4, 4: 6, 5: 7}


def rows_of(start, size):
    return pl.ds(pl.multiple_of(start, SLICE), size)


def kernel(
    q_hbm, k_hbm, v_hbm, ld_hbm, lw_hbm, skip_hbm, gain_hbm, out_ref,
    q_ref, k_ref, v_ref, ld_ref, lw_ref, skip_ref, gain_ref, in_sem,
    lc_ref, lct_ref, w0_ref, ci_ref, cum_ref, coef_ref, vt_ref, rb_ref, st_ref, acc_ref, y_ref,
    comb_ref, pcomb_ref, fall_ref, pair_ref, crow_ref, crows_ref,
    gath_ref, node_ref, bucket_ref, qt_ref, bb_ref, sq_ref, sqs_ref,
    ex_ss, ex_rs, cb_ss, cb_rs, l0_ss, l0_rs, cr_ss, cr_rs, p1_ss, p1_rs, n1_ss, n1_rs,
    p2_ss, p2_rs, z_ss, z_rs, fw_ss, fw_rs, sq_ss, sq_rs, here_z, here_h,
):
    seq = lax.axis_index("seq")
    head = lax.axis_index("head")
    zhi = seq // PLANE
    me = seq % PLANE
    chip = me // 2
    core = me % 2
    base = zhi * PLANE
    bits = [core] + [(chip // (1 << b)) % 2 for b in range(4)] + [zhi]

    def at(s):
        return {"seq": s, "head": head}

    def same_core(to):
        return at(base + 2 * to + core)

    def remote(src, dst, ss, rs, device):
        return pltpu.make_async_remote_copy(
            src_ref=src, dst_ref=dst, send_sem=ss, recv_sem=rs,
            device_id=device, device_id_type=pl.DeviceIdType.MESH,
        )

    partner = at(base + me + 1 - 2 * core)
    zpeer = at(seq + PLANE - 2 * PLANE * zhi)
    half = rows_of(HALF * core, HALF)
    other = rows_of(HALF * (1 - core), HALF)
    mine = HALF * core + SLICE * chip

    pairs = [(ld_hbm, ld_ref), (k_hbm, k_ref), (lw_hbm, lw_ref), (q_hbm, q_ref),
             (skip_hbm, skip_ref), (gain_hbm, gain_ref)]
    loads = [pltpu.make_async_copy(src, dst, in_sem.at[i]) for i, (src, dst) in enumerate(pairs)]
    loads[0].start()
    for c in range(NC):
        pltpu.make_async_copy(v_hbm.at[c], v_ref.at[c], in_sem.at[6 + c]).start()
    for copy in loads[1:]:
        copy.start()

    barrier = pltpu.get_barrier_semaphore()

    def greet(device, sem=barrier):
        pl.semaphore_signal(sem, inc=1, device_id=device, device_id_type=pl.DeviceIdType.MESH)

    def rank_of(h):
        return h + zhi * (GROUP - 1 - 2 * h)

    def peer(r):
        return (head + r) % GROUP

    rank = rank_of(head)

    @pl.loop(1, CHIPS)
    def _(r):
        greet(same_core((chip + r) % CHIPS))

    greet(partner)

    @pl.when(zhi == 0)
    def _():
        greet(zpeer)

    @pl.loop(1, GROUP)
    def _(r):
        @pl.when(rank_of(peer(r)) > rank)
        def _():
            greet({"seq": seq, "head": peer(r)})

    loads[0].wait()
    row = lax.broadcasted_iota(jnp.int32, (CH, CH), 0)
    col = lax.broadcasted_iota(jnp.int32, (CH, CH), 1)
    tri = jnp.where(row <= col, 1.0, 0.0).astype(BF16)
    his, mids, los = [], [], []
    for c in range(NC):
        x = ld_ref[:, c * CH:(c + 1) * CH]
        hi = x.astype(BF16)
        rest = x - hi.astype(F32)
        mid = rest.astype(BF16)
        his.append(hi)
        mids.append(mid)
        los.append((rest - mid.astype(F32)).astype(BF16))
    sums = jnp.dot(jnp.concatenate(his + mids + los, axis=0), tri, preferred_element_type=F32)
    n = HEADS * NC
    total = jnp.zeros((HEADS, CH), F32)
    trow = jnp.zeros((1, CH), F32)
    for c in range(NC):
        a = HEADS * c
        lc = sums[a:a + HEADS] + sums[n + a:n + a + HEADS] + sums[2 * n + a:2 * n + a + HEADS]
        lc_ref[c] = lc
        cum_ref[c] = lc + total
        turned = jnp.concatenate([lc, jnp.zeros((CH - HEADS, CH), F32)], axis=0).T
        lct_ref[c] = turned
        trow = trow + turned[CH - 1:CH]
        total = total + jnp.broadcast_to(lc[:, CH - 1:CH], (HEADS, CH))
    comb_ref[0:HEADS] = total
    comb_ref[HEADS:HEADS + 8] = jnp.broadcast_to(trow, (8, CH))

    st_ref[...] = jnp.zeros((ROWS, STATE), F32)
    loads[1].wait()

    @pl.loop(0, NC)
    def _(c):
        pltpu.make_async_copy(v_hbm.at[c], v_ref.at[c], in_sem.at[6 + c]).wait()
        lc = lc_ref[c]
        last = jnp.broadcast_to(lc[:, CH - 1:CH], (HEADS, CH))
        fall = jnp.exp(last)
        tail = jnp.exp(last - lc)
        scaled = []
        for j in range(ROWS // CH):
            vt = v_ref[c, :, j * CH:(j + 1) * CH].T
            vt_ref[c, j * CH:(j + 1) * CH, :] = vt
            wide = vt.astype(F32)
            for i in range(2):
                h = 2 * j + i
                scaled.append((wide[i * DIM:(i + 1) * DIM] * tail[h:h + 1]).astype(BF16))
        new = jnp.dot(jnp.concatenate(scaled, axis=0), k_ref[c], preferred_element_type=F32)
        for h in range(HEADS):
            rows = slice(h * DIM, (h + 1) * DIM)
            old = st_ref[rows]
            rb_ref[c, rows] = old.astype(BF16)
            st_ref[rows] = fall[h:h + 1] * old + new[rows]

    pl.semaphore_wait(barrier, CHIPS - 1 + 1 + rank + zhi)

    swap = remote(st_ref.at[other], bucket_ref.at[0, other], ex_ss, ex_rs, partner)
    comb = remote(comb_ref, pcomb_ref, cb_ss, cb_rs, partner)
    zero = remote(st_ref.at[half], bucket_ref.at[0, half], l0_ss, l0_rs, partner)
    swap.start()
    comb.start()

    @pl.when(zhi == 1)
    def _():
        greet(zpeer, here_z)

    @pl.loop(1, GROUP)
    def _(r):
        @pl.when(rank_of(peer(r)) < rank)
        def _():
            greet({"seq": seq, "head": peer(r)}, here_h)

    loads[2].wait()
    for copy in loads[3:]:
        copy.wait()
    for c in range(NC):
        w0 = lw_ref[0, :, c * CH:(c + 1) * CH].astype(F32)
        w0_ref[c] = w0
        ci_ref[c] = w0 * jnp.exp(lc_ref[c])
        qt_ref[c // 2, :, (c % 2) * CH:(c % 2 + 1) * CH] = q_ref[c].T

    def inside(first, last):
        @pl.loop(first, last)
        def _(c):
            qc = q_ref[c]
            s = lax.dot_general(k_ref[c], qc, NT, preferred_element_type=F32)
            r0 = lax.broadcasted_iota(jnp.int32, (CH, CH), 0)
            c0 = lax.broadcasted_iota(jnp.int32, (CH, CH), 1)
            s = jnp.where(r0 <= c0, s, 0.0)
            inter = lax.dot_general(rb_ref[c], qc, NT, preferred_element_type=F32)
            for h in range(HEADS):
                rows = slice(h * DIM, (h + 1) * DIM)
                d = jnp.minimum(lc_ref[c, h:h + 1] - lct_ref[c, :, h:h + 1], 0.0)
                mix = (jnp.exp(d) * s).astype(BF16)
                vt = vt_ref[c, rows]
                o = jnp.dot(vt, mix, preferred_element_type=F32)
                acc_ref[c, rows] = (
                    w0_ref[c, h:h + 1] * o + ci_ref[c, h:h + 1] * inter[rows]
                    + skip_ref[h] * vt.astype(F32))

    inside(0, 2)

    comb.wait_recv()
    remote(st_ref.at[half], bucket_ref.at[0, half], ex_ss, ex_rs, partner).wait_recv()
    late = jnp.where(core == 0, pcomb_ref[0:HEADS], comb_ref[0:HEADS])
    fall_ref[...] = jnp.exp(late)
    for i in range(HH):
        at_head = rows_of(HALF * core + DIM * i, DIM)
        own, got = st_ref[at_head], bucket_ref[0, at_head]
        left = jnp.where(core == 0, own, got)
        right = jnp.where(core == 0, got, own)
        pair_ref[i * DIM:(i + 1) * DIM] = fall_ref[pl.ds(HH * core + i, 1), :] * left + right
    crow = comb_ref[HEADS:HEADS + 1] + pcomb_ref[HEADS:HEADS + 1]
    crow_ref[...] = crow
    crows_ref[chip] = crow

    @pl.loop(1, CHIPS)
    def _(r):
        to = (chip + r) % CHIPS
        remote(pair_ref.at[rows_of(SLICE * to, SLICE)], gath_ref.at[chip], p1_ss, p1_rs,
               same_core(to)).start()
        remote(crow_ref, crows_ref.at[chip], cr_ss, cr_rs, same_core(to)).start()

    @pl.when(core == 0)
    def _():
        zero.start()

    first_level = remote(
        pair_ref, bucket_ref.at[1, half], n1_ss, n1_rs, same_core(chip + 1 - 2 * bits[1]))

    @pl.when(bits[1] == 0)
    def _():
        first_level.start()

    gath_ref[chip] = pair_ref[rows_of(SLICE * chip, SLICE)]

    inside(2, NC)

    fifteen = pl.ds(0, CHIPS - 1)
    crs = remote(crows_ref.at[fifteen], crows_ref.at[fifteen], cr_ss, cr_rs, partner)
    p1s = remote(gath_ref.at[fifteen], gath_ref.at[fifteen], p1_ss, p1_rs, partner)
    crs.wait_recv()
    p1s.wait_recv()

    lane = lax.broadcasted_iota(jnp.int32, (1, CH), 1)
    pick = lane == HH * core + chip // 2
    nodes = [gath_ref[i] for i in range(CHIPS)]
    weights = [
        jnp.sum(jnp.where(pick, crows_ref[i], 0.0), axis=1, keepdims=True) for i in range(CHIPS)]
    slot = 0
    for level in range(2, LEVELS):
        count = len(nodes) // 2
        joined = [
            jnp.exp(jnp.broadcast_to(weights[2 * j + 1], (1, CH))) * nodes[2 * j] + nodes[2 * j + 1]
            for j in range(count)
        ]
        weights = [weights[2 * j] + weights[2 * j + 1] for j in range(count)]
        nodes = joined
        for j in range(0, count, 2):
            node_ref[slot] = nodes[j]
            slot += 1

    up = remote(
        node_ref.at[STARTS[5]], bucket_ref.at[5, rows_of(mine, SLICE)], z_ss, z_rs, zpeer)

    for level in range(2, 5):
        @pl.loop(1, CHIPS)
        def _(r):
            to = (chip + r) % CHIPS

            @pl.when((to // (1 << (level - 1))) % 2 == 1)
            def _():
                remote(
                    node_ref.at[STARTS[level] + to // (1 << level)],
                    bucket_ref.at[level, rows_of(mine, SLICE)],
                    p2_ss.at[level], p2_rs.at[level], same_core(to)).start()

    @pl.when(zhi == 0)
    def _():
        pl.semaphore_wait(here_z, 1)
        up.start()

    for level in range(2, 5):
        @pl.when(bits[level] == 1)
        def _():
            bucket_ref[level, rows_of(mine, SLICE)] = node_ref[STARTS[level] + chip // (1 << level)]

    before = [jnp.zeros((1, CH), F32) for _ in range(LEVELS)]
    for i in range(CHIPS - 1):
        t = crows_ref[i]
        for level in range(2, LEVELS):
            counts = (i < chip) & (i >= chip - chip % (1 << (level - 1)))
            before[level] = before[level] + jnp.where(counts, t, 0.0)
    turned = jnp.concatenate(before + [jnp.zeros((CH - LEVELS, CH), F32)], axis=0).T
    inner = jnp.where(core == 1, pcomb_ref[0:HEADS], 0.0)
    for level in range(LEVELS):
        off = jnp.zeros((HEADS, CH), F32)
        if level > 0:
            off = inner
        if level > 1:
            off = off + jnp.broadcast_to(turned[0:HEADS, level:level + 1], (HEADS, CH))
        for c in range(NC):
            w = lw_ref[level + 1, :, c * CH:(c + 1) * CH].astype(F32)
            coef_ref[level, c] = w * jnp.exp(cum_ref[c] + off)

    def cross(level, side):
        at_half = rows_of(HALF * side, HALF)
        bb_ref[...] = bucket_ref[level, at_half].astype(BF16)

        for d in range(NC // 2):
            o = jnp.dot(bb_ref[...], qt_ref[d], preferred_element_type=F32)
            for i in range(2):
                c = 2 * d + i
                for h in range(HH):
                    rows = rows_of(HALF * side + DIM * h, DIM)
                    acc_ref[c, rows] = (
                        acc_ref[c, rows]
                        + coef_ref[level, c, pl.ds(HH * side + h, 1), :]
                        * o[h * DIM:(h + 1) * DIM, i * CH:(i + 1) * CH])

    def forward(level):
        return remote(
            bucket_ref.at[level, half], bucket_ref.at[level, half],
            fw_ss.at[level], fw_rs.at[level], partner)

    def forwarded(level):
        return remote(
            bucket_ref.at[level, other], bucket_ref.at[level, other],
            fw_ss.at[level], fw_rs.at[level], partner)

    some = pl.ds(0, (CHIPS - 1) * SLICE)

    def slices(level):
        part = bucket_ref.at[level, some]
        return remote(part, part, p2_ss.at[level], p2_rs.at[level], partner)

    @pl.when(core == 1)
    def _():
        cross(0, core)
        remote(st_ref.at[other], bucket_ref.at[0, other], l0_ss, l0_rs, partner).wait_recv()
        cross(0, 1 - core)

    @pl.when(zhi == 1)
    def _():
        up.wait_recv()
        own = bucket_ref.at[5, rows_of(mine, SLICE)]

        @pl.loop(1, CHIPS)
        def _(r):
            remote(own, own, p2_ss.at[5], p2_rs.at[5], same_core((chip + r) % CHIPS)).start()

    @pl.when(bits[1] == 1)
    def _():
        first_level.wait_recv()
        forward(1).start()
        cross(1, core)
        forwarded(1).wait_recv()
        cross(1, 1 - core)

    for level in range(2, 5):
        @pl.when(bits[level] == 1)
        def _():
            slices(level).wait_recv()
            forward(level).start()
            cross(level, core)

    def rest(level):
        @pl.when(bits[level] == 1)
        def _():
            forwarded(level).wait_recv()
            cross(level, 1 - core)

    rest(2)

    @pl.when(zhi == 1)
    def _():
        slices(5).wait_recv()
        forward(5).start()
        cross(5, core)

    for level in range(3, LEVELS):
        rest(level)

    sq_ref[...] = jnp.zeros((8, CH), F32)
    for c in range(NC):
        y = acc_ref[c]
        sq_ref[c:c + 1] = jnp.sum(y * y, axis=0, keepdims=True)
    sqs_ref[head] = sq_ref[...]

    @pl.when(rank < GROUP - 1)
    def _():
        pl.semaphore_wait(here_h, GROUP - 1 - rank)

    @pl.loop(1, GROUP)
    def _(r):
        remote(
            sq_ref, sqs_ref.at[head], sq_ss, sq_rs,
            {"seq": seq, "head": (head + r) % GROUP}).start()

    gain = gain_ref[...].reshape(1, ROWS).astype(F32)

    @pl.loop(0, NC)
    def _(c):
        for j in range(ROWS // CH):
            cols = slice(j * CH, (j + 1) * CH)
            y_ref[c, :, cols] = acc_ref[c, cols].T * gain[:, cols]

    swap.wait_send()
    comb.wait_send()
    crs.wait_send()
    p1s.wait_send()

    @pl.when(core == 0)
    def _():
        zero.wait_send()

    @pl.when(bits[1] == 0)
    def _():
        first_level.wait_send()

    @pl.when(bits[1] == 1)
    def _():
        forward(1).wait_send()

    for level in range(2, 5):
        for has in range(2):
            @pl.when(bits[level] == has)
            def _():
                sent = bucket_ref.at[level, pl.ds(0, (CHIPS // 2 - has) * SLICE)]
                remote(sent, sent, p2_ss.at[level], p2_rs.at[level], partner).wait_send()

        @pl.when(bits[level] == 1)
        def _():
            forward(level).wait_send()

    @pl.when(zhi == 0)
    def _():
        up.wait_send()

    @pl.when(zhi == 1)
    def _():
        slices(5).wait_send()
        forward(5).wait_send()

    seven = sqs_ref.at[pl.ds(0, GROUP - 1)]
    remote(seven, seven, sq_ss, sq_rs, partner).wait_recv()
    remote(seven, seven, sq_ss, sq_rs, partner).wait_send()

    whole = sqs_ref[0]
    for g in range(1, GROUP):
        whole = whole + sqs_ref[g]
    inv = lax.rsqrt(whole / CHANNELS + 1e-05)
    turned = jnp.concatenate([inv, jnp.zeros((CH - 8, CH), F32)], axis=0).T
    for c in range(NC):
        out_ref[c] = (y_ref[c] * turned[:, c:c + 1]).astype(BF16)


def shards(queries, keys, values, log_decay, level_weight, skip, norm_gain):
    hbm = pl.BlockSpec(memory_space=pltpu.HBM)
    dma = pltpu.SemaphoreType.DMA

    def stay(x):
        return pltpu.with_memory_space_constraint(x, pltpu.HBM)

    out = pl.pallas_call(
        kernel,
        out_shape=jax.ShapeDtypeStruct((NC, CH, ROWS), BF16),
        in_specs=[hbm] * 7,
        out_specs=pl.BlockSpec(memory_space=pltpu.VMEM),
        scratch_shapes=[
            pltpu.VMEM((NC, CH, STATE), BF16),
            pltpu.VMEM((NC, CH, STATE), BF16),
            pltpu.VMEM((NC, CH, ROWS), BF16),
            pltpu.VMEM((HEADS, TOK), F32),
            pltpu.VMEM((LEVELS + 1, HEADS, TOK), BF16),
            pltpu.SMEM((HEADS,), F32),
            pltpu.VMEM((ROWS,), BF16),
            dma((6 + NC,)),
            pltpu.VMEM((NC, HEADS, CH), F32),
            pltpu.VMEM((NC, CH, CH), F32),
            pltpu.VMEM((NC, HEADS, CH), F32),
            pltpu.VMEM((NC, HEADS, CH), F32),
            pltpu.VMEM((NC, HEADS, CH), F32),
            pltpu.VMEM((LEVELS, NC, HEADS, CH), F32),
            pltpu.VMEM((NC, ROWS, CH), BF16),
            pltpu.VMEM((NC, ROWS, STATE), BF16),
            pltpu.VMEM((ROWS, STATE), F32),
            pltpu.VMEM((NC, ROWS, CH), F32),
            pltpu.VMEM((NC, CH, ROWS), F32),
            pltpu.VMEM((HEADS + 8, CH), F32),
            pltpu.VMEM((HEADS + 8, CH), F32),
            pltpu.VMEM((HEADS, CH), F32),
            pltpu.VMEM((HALF, STATE), F32),
            pltpu.VMEM((1, CH), F32),
            pltpu.VMEM((CHIPS, 1, CH), F32),
            pltpu.VMEM((CHIPS, SLICE, STATE), F32),
            pltpu.VMEM((8, SLICE, STATE), F32),
            pltpu.VMEM((LEVELS, ROWS, STATE), F32),
            pltpu.VMEM((NC // 2, STATE, 2 * CH), BF16),
            pltpu.VMEM((HALF, STATE), BF16),
            pltpu.VMEM((8, CH), F32),
            pltpu.VMEM((GROUP, 8, CH), F32),
            dma, dma, dma, dma, dma, dma, dma, dma, dma, dma, dma, dma,
            dma((LEVELS,)), dma((LEVELS,)), dma, dma, dma((LEVELS,)), dma((LEVELS,)), dma, dma,
            pltpu.SemaphoreType.REGULAR, pltpu.SemaphoreType.REGULAR,
        ],
        compiler_params=pltpu.CompilerParams(
            collective_id=0, has_side_effects=True, vmem_limit_bytes=50 << 20),
        name="layer",
    )(
        stay(queries.reshape(NC, CH, STATE)), stay(keys.reshape(NC, CH, STATE)),
        stay(values.reshape(NC, CH, ROWS)), stay(log_decay), stay(level_weight), stay(skip),
        stay(norm_gain),
    )
    return out.reshape(TOK, ROWS)


def solution(mesh):
    placed = (
        P("seq", None), P("seq", None), P("seq", "head"), P("head", "seq"),
        P(None, "head", "seq"), P("head"), P("head"),
    )
    return jax.shard_map(
        shards, mesh=mesh, in_specs=placed, out_specs=P("seq", "head"), check_vma=False
    )
```

```python
import jax
import jax.numpy as jnp
from jax import lax
from jax.experimental import pallas as pl
from jax.experimental.pallas import tpu as pltpu
from jax.sharding import PartitionSpec as P

F32 = jnp.float32
BF16 = jnp.bfloat16
NT = (((1,), (1,)), ((), ()))

TOK = 768
CH = 128
NC = TOK // CH
HEADS = 16
HH = HEADS // 2
DIM = 64
STATE = 128
ROWS = HEADS * DIM
HALF = ROWS // 2
PLANE = 32
CHIPS = 16
SLICE = HALF // CHIPS
LEVELS = 6
GROUP = 8
CHANNELS = 8192
STARTS = {2: 0, 3: 4, 4: 6, 5: 7}
SIDE = 4
STEPS = sorted(
    ((dx, dy) for dx in range(SIDE) for dy in range(SIDE) if dx + dy > 0),
    key=lambda d: -min(d[0], SIDE - d[0]) - min(d[1], SIDE - d[1]))


def rows_of(start, size):
    return pl.ds(pl.multiple_of(start, SLICE), size)


def kernel(
    q_hbm, k_hbm, v_hbm, ld_hbm, lw_hbm, skip_hbm, gain_hbm, out_ref,
    q_ref, k_ref, v_ref, ld_ref, lw_ref, skip_ref, gain_ref, in_sem,
    lc_ref, lct_ref, w0_ref, ci_ref, cum_ref, coef_ref, vt_ref, rb_ref, st_ref, acc_ref, y_ref,
    comb_ref, pcomb_ref, fall_ref, pair_ref, crow_ref, crows_ref,
    gath_ref, node_ref, bucket_ref, qt_ref, bb_ref, sq_ref, sqs_ref,
    ex_ss, ex_rs, cb_ss, cb_rs, l0_ss, l0_rs, cr_ss, cr_rs, p1_ss, p1_rs, n1_ss, n1_rs,
    p2_ss, p2_rs, z_ss, z_rs, fw_ss, fw_rs, sq_ss, sq_rs, here_z, here_h,
):
    seq = lax.axis_index("seq")
    head = lax.axis_index("head")
    zhi = seq // PLANE
    me = seq % PLANE
    chip = me // 2
    core = me % 2
    base = zhi * PLANE
    bits = [core] + [(chip // (1 << b)) % 2 for b in range(4)] + [zhi]

    def at(s):
        return {"seq": s, "head": head}

    cx = chip % SIDE
    cy = chip // SIDE

    def away(step):
        return SIDE * ((cy + step[1]) % SIDE) + (cx + step[0]) % SIDE

    def same_core(to):
        return at(base + 2 * to + core)

    def remote(src, dst, ss, rs, device):
        return pltpu.make_async_remote_copy(
            src_ref=src, dst_ref=dst, send_sem=ss, recv_sem=rs,
            device_id=device, device_id_type=pl.DeviceIdType.MESH,
        )

    partner = at(base + me + 1 - 2 * core)
    zpeer = at(seq + PLANE - 2 * PLANE * zhi)
    half = rows_of(HALF * core, HALF)
    other = rows_of(HALF * (1 - core), HALF)
    mine = HALF * core + SLICE * chip

    pairs = [(ld_hbm, ld_ref), (k_hbm, k_ref), (lw_hbm, lw_ref), (q_hbm, q_ref),
             (skip_hbm, skip_ref), (gain_hbm, gain_ref)]
    loads = [pltpu.make_async_copy(src, dst, in_sem.at[i]) for i, (src, dst) in enumerate(pairs)]
    loads[0].start()
    for c in range(NC):
        pltpu.make_async_copy(v_hbm.at[c], v_ref.at[c], in_sem.at[6 + c]).start()
    for copy in loads[1:]:
        copy.start()

    barrier = pltpu.get_barrier_semaphore()

    def greet(device, sem=barrier):
        pl.semaphore_signal(sem, inc=1, device_id=device, device_id_type=pl.DeviceIdType.MESH)

    def rank_of(h):
        return h + zhi * (GROUP - 1 - 2 * h)

    def peer(r):
        return (head + r) % GROUP

    rank = rank_of(head)

    for step in STEPS:
        greet(same_core(away(step)))

    greet(partner)

    @pl.when(zhi == 0)
    def _():
        greet(zpeer)

    @pl.loop(1, GROUP)
    def _(r):
        @pl.when(rank_of(peer(r)) > rank)
        def _():
            greet({"seq": seq, "head": peer(r)})

    loads[0].wait()
    row = lax.broadcasted_iota(jnp.int32, (CH, CH), 0)
    col = lax.broadcasted_iota(jnp.int32, (CH, CH), 1)
    tri = jnp.where(row <= col, 1.0, 0.0).astype(BF16)
    his, mids, los = [], [], []
    for c in range(NC):
        x = ld_ref[:, c * CH:(c + 1) * CH]
        hi = x.astype(BF16)
        rest = x - hi.astype(F32)
        mid = rest.astype(BF16)
        his.append(hi)
        mids.append(mid)
        los.append((rest - mid.astype(F32)).astype(BF16))
    sums = jnp.dot(jnp.concatenate(his + mids + los, axis=0), tri, preferred_element_type=F32)
    n = HEADS * NC
    total = jnp.zeros((HEADS, CH), F32)
    trow = jnp.zeros((1, CH), F32)
    for c in range(NC):
        a = HEADS * c
        lc = sums[a:a + HEADS] + sums[n + a:n + a + HEADS] + sums[2 * n + a:2 * n + a + HEADS]
        lc_ref[c] = lc
        cum_ref[c] = lc + total
        turned = jnp.concatenate([lc, jnp.zeros((CH - HEADS, CH), F32)], axis=0).T
        lct_ref[c] = turned
        trow = trow + turned[CH - 1:CH]
        total = total + jnp.broadcast_to(lc[:, CH - 1:CH], (HEADS, CH))
    comb_ref[0:HEADS] = total
    comb_ref[HEADS:HEADS + 8] = jnp.broadcast_to(trow, (8, CH))

    st_ref[...] = jnp.zeros((ROWS, STATE), F32)
    loads[1].wait()

    @pl.loop(0, NC)
    def _(c):
        pltpu.make_async_copy(v_hbm.at[c], v_ref.at[c], in_sem.at[6 + c]).wait()
        lc = lc_ref[c]
        last = jnp.broadcast_to(lc[:, CH - 1:CH], (HEADS, CH))
        fall = jnp.exp(last)
        tail = jnp.exp(last - lc)
        scaled = []
        for j in range(ROWS // CH):
            vt = v_ref[c, :, j * CH:(j + 1) * CH].T
            vt_ref[c, j * CH:(j + 1) * CH, :] = vt
            wide = vt.astype(F32)
            for i in range(2):
                h = 2 * j + i
                scaled.append((wide[i * DIM:(i + 1) * DIM] * tail[h:h + 1]).astype(BF16))
        new = jnp.dot(jnp.concatenate(scaled, axis=0), k_ref[c], preferred_element_type=F32)
        for h in range(HEADS):
            rows = slice(h * DIM, (h + 1) * DIM)
            old = st_ref[rows]
            rb_ref[c, rows] = old.astype(BF16)
            st_ref[rows] = fall[h:h + 1] * old + new[rows]

    pl.semaphore_wait(barrier, CHIPS - 1 + 1 + rank + zhi)

    swap = remote(st_ref.at[other], bucket_ref.at[0, other], ex_ss, ex_rs, partner)
    comb = remote(comb_ref, pcomb_ref, cb_ss, cb_rs, partner)
    zero = remote(st_ref.at[half], bucket_ref.at[0, half], l0_ss, l0_rs, partner)
    swap.start()
    comb.start()

    @pl.when(zhi == 1)
    def _():
        greet(zpeer, here_z)

    @pl.loop(1, GROUP)
    def _(r):
        @pl.when(rank_of(peer(r)) < rank)
        def _():
            greet({"seq": seq, "head": peer(r)}, here_h)

    loads[2].wait()
    for copy in loads[3:]:
        copy.wait()
    for c in range(NC):
        w0 = lw_ref[0, :, c * CH:(c + 1) * CH].astype(F32)
        w0_ref[c] = w0
        ci_ref[c] = w0 * jnp.exp(lc_ref[c])
        qt_ref[c // 2, :, (c % 2) * CH:(c % 2 + 1) * CH] = q_ref[c].T

    def inside(first, last):
        @pl.loop(first, last)
        def _(c):
            qc = q_ref[c]
            s = lax.dot_general(k_ref[c], qc, NT, preferred_element_type=F32)
            r0 = lax.broadcasted_iota(jnp.int32, (CH, CH), 0)
            c0 = lax.broadcasted_iota(jnp.int32, (CH, CH), 1)
            s = jnp.where(r0 <= c0, s, 0.0)
            inter = lax.dot_general(rb_ref[c], qc, NT, preferred_element_type=F32)
            for h in range(HEADS):
                rows = slice(h * DIM, (h + 1) * DIM)
                d = jnp.minimum(lc_ref[c, h:h + 1] - lct_ref[c, :, h:h + 1], 0.0)
                mix = (jnp.exp(d) * s).astype(BF16)
                vt = vt_ref[c, rows]
                o = jnp.dot(vt, mix, preferred_element_type=F32)
                acc_ref[c, rows] = (
                    w0_ref[c, h:h + 1] * o + ci_ref[c, h:h + 1] * inter[rows]
                    + skip_ref[h] * vt.astype(F32))

    inside(0, 2)

    comb.wait_recv()
    remote(st_ref.at[half], bucket_ref.at[0, half], ex_ss, ex_rs, partner).wait_recv()
    late = jnp.where(core == 0, pcomb_ref[0:HEADS], comb_ref[0:HEADS])
    fall_ref[...] = jnp.exp(late)
    for i in range(HH):
        at_head = rows_of(HALF * core + DIM * i, DIM)
        own, got = st_ref[at_head], bucket_ref[0, at_head]
        left = jnp.where(core == 0, own, got)
        right = jnp.where(core == 0, got, own)
        pair_ref[i * DIM:(i + 1) * DIM] = fall_ref[pl.ds(HH * core + i, 1), :] * left + right
    crow = comb_ref[HEADS:HEADS + 1] + pcomb_ref[HEADS:HEADS + 1]
    crow_ref[...] = crow
    crows_ref[chip] = crow

    for step in STEPS:
        to = away(step)
        remote(pair_ref.at[rows_of(SLICE * to, SLICE)], gath_ref.at[chip], p1_ss, p1_rs,
               same_core(to)).start()
        remote(crow_ref, crows_ref.at[chip], cr_ss, cr_rs, same_core(to)).start()

    @pl.when(core == 0)
    def _():
        zero.start()

    first_level = remote(
        pair_ref, bucket_ref.at[1, half], n1_ss, n1_rs, same_core(chip + 1 - 2 * bits[1]))

    gath_ref[chip] = pair_ref[rows_of(SLICE * chip, SLICE)]

    inside(2, NC)

    @pl.when(bits[1] == 0)
    def _():
        first_level.start()

    fifteen = pl.ds(0, CHIPS - 1)
    crs = remote(crows_ref.at[fifteen], crows_ref.at[fifteen], cr_ss, cr_rs, partner)
    p1s = remote(gath_ref.at[fifteen], gath_ref.at[fifteen], p1_ss, p1_rs, partner)
    crs.wait_recv()
    p1s.wait_recv()

    lane = lax.broadcasted_iota(jnp.int32, (1, CH), 1)
    pick = lane == HH * core + chip // 2
    nodes = [gath_ref[i] for i in range(CHIPS)]
    weights = [
        jnp.sum(jnp.where(pick, crows_ref[i], 0.0), axis=1, keepdims=True) for i in range(CHIPS)]
    slot = 0
    for level in range(2, LEVELS):
        count = len(nodes) // 2
        joined = [
            jnp.exp(jnp.broadcast_to(weights[2 * j + 1], (1, CH))) * nodes[2 * j] + nodes[2 * j + 1]
            for j in range(count)
        ]
        weights = [weights[2 * j] + weights[2 * j + 1] for j in range(count)]
        nodes = joined
        for j in range(0, count, 2):
            node_ref[slot] = nodes[j]
            slot += 1

    up = remote(
        node_ref.at[STARTS[5]], bucket_ref.at[5, rows_of(mine, SLICE)], z_ss, z_rs, zpeer)

    for level in range(2, 5):
        for step in STEPS:
            to = away(step)

            @pl.when((to // (1 << (level - 1))) % 2 == 1)
            def _():
                remote(
                    node_ref.at[STARTS[level] + to // (1 << level)],
                    bucket_ref.at[level, rows_of(mine, SLICE)],
                    p2_ss.at[level], p2_rs.at[level], same_core(to)).start()

    @pl.when(zhi == 0)
    def _():
        pl.semaphore_wait(here_z, 1)
        up.start()

    for level in range(2, 5):
        @pl.when(bits[level] == 1)
        def _():
            bucket_ref[level, rows_of(mine, SLICE)] = node_ref[STARTS[level] + chip // (1 << level)]

    before = [jnp.zeros((1, CH), F32) for _ in range(LEVELS)]
    for i in range(CHIPS - 1):
        t = crows_ref[i]
        for level in range(2, LEVELS):
            counts = (i < chip) & (i >= chip - chip % (1 << (level - 1)))
            before[level] = before[level] + jnp.where(counts, t, 0.0)
    turned = jnp.concatenate(before + [jnp.zeros((CH - LEVELS, CH), F32)], axis=0).T
    inner = jnp.where(core == 1, pcomb_ref[0:HEADS], 0.0)
    for level in range(LEVELS):
        off = jnp.zeros((HEADS, CH), F32)
        if level > 0:
            off = inner
        if level > 1:
            off = off + jnp.broadcast_to(turned[0:HEADS, level:level + 1], (HEADS, CH))
        for c in range(NC):
            w = lw_ref[level + 1, :, c * CH:(c + 1) * CH].astype(F32)
            coef_ref[level, c] = w * jnp.exp(cum_ref[c] + off)

    def cross(level, side):
        at_half = rows_of(HALF * side, HALF)
        bb_ref[...] = bucket_ref[level, at_half].astype(BF16)

        for d in range(NC // 2):
            o = jnp.dot(bb_ref[...], qt_ref[d], preferred_element_type=F32)
            for i in range(2):
                c = 2 * d + i
                for h in range(HH):
                    rows = rows_of(HALF * side + DIM * h, DIM)
                    acc_ref[c, rows] = (
                        acc_ref[c, rows]
                        + coef_ref[level, c, pl.ds(HH * side + h, 1), :]
                        * o[h * DIM:(h + 1) * DIM, i * CH:(i + 1) * CH])

    def forward(level):
        return remote(
            bucket_ref.at[level, half], bucket_ref.at[level, half],
            fw_ss.at[level], fw_rs.at[level], partner)

    def forwarded(level):
        return remote(
            bucket_ref.at[level, other], bucket_ref.at[level, other],
            fw_ss.at[level], fw_rs.at[level], partner)

    some = pl.ds(0, (CHIPS - 1) * SLICE)

    def slices(level):
        part = bucket_ref.at[level, some]
        return remote(part, part, p2_ss.at[level], p2_rs.at[level], partner)

    @pl.when(core == 1)
    def _():
        cross(0, 1)
        remote(st_ref.at[other], bucket_ref.at[0, other], l0_ss, l0_rs, partner).wait_recv()
        cross(0, 0)

    @pl.when(zhi == 1)
    def _():
        up.wait_recv()
        own = bucket_ref.at[5, rows_of(mine, SLICE)]

        for step in STEPS:
            remote(own, own, p2_ss.at[5], p2_rs.at[5], same_core(away(step))).start()

    @pl.when(bits[1] == 1)
    def _():
        first_level.wait_recv()
        forward(1).start()
        cross(1, core)
        forwarded(1).wait_recv()
        cross(1, 1 - core)

    def landed(level):
        slices(level).wait_recv()
        forward(level).start()

    def rest(level):
        forwarded(level).wait_recv()
        cross(level, 1 - core)

    @pl.when(bits[2] == 1)
    def _():
        landed(2)
        cross(2, core)

    @pl.when((bits[2] == 1) & (core == 0))
    def _():
        rest(2)

    for level in range(3, 5):
        @pl.when(bits[level] == 1)
        def _():
            landed(level)

    for level in range(3, 5):
        @pl.when(bits[level] == 1)
        def _():
            cross(level, core)

    @pl.when((bits[2] == 1) & (core == 1))
    def _():
        rest(2)

    @pl.when(zhi == 1)
    def _():
        landed(5)
        cross(5, core)

    sq_ref[...] = jnp.zeros((8, CH), F32)

    def squares(c, rows):
        y = acc_ref[c, rows]
        return jnp.sum(y * y, axis=0, keepdims=True)

    for c in range(NC):
        sq_ref[c:c + 1] = squares(c, half)

    for level in range(3, LEVELS):
        @pl.when(bits[level] == 1)
        def _():
            rest(level)

    for c in range(NC):
        sq_ref[c:c + 1] = sq_ref[c:c + 1] + squares(c, other)
    sqs_ref[head] = sq_ref[...]

    @pl.when(rank < GROUP - 1)
    def _():
        pl.semaphore_wait(here_h, GROUP - 1 - rank)

    @pl.loop(1, GROUP)
    def _(r):
        remote(
            sq_ref, sqs_ref.at[head], sq_ss, sq_rs,
            {"seq": seq, "head": (head + r) % GROUP}).start()

    gain = gain_ref[...].reshape(1, ROWS).astype(F32)

    @pl.loop(0, NC)
    def _(c):
        for j in range(ROWS // CH):
            cols = slice(j * CH, (j + 1) * CH)
            y_ref[c, :, cols] = acc_ref[c, cols].T * gain[:, cols]

    swap.wait_send()
    comb.wait_send()
    crs.wait_send()
    p1s.wait_send()

    @pl.when(core == 0)
    def _():
        zero.wait_send()

    @pl.when(bits[1] == 0)
    def _():
        first_level.wait_send()

    @pl.when(bits[1] == 1)
    def _():
        forward(1).wait_send()

    for level in range(2, 5):
        for has in range(2):
            @pl.when(bits[level] == has)
            def _():
                sent = bucket_ref.at[level, pl.ds(0, (CHIPS // 2 - has) * SLICE)]
                remote(sent, sent, p2_ss.at[level], p2_rs.at[level], partner).wait_send()

        @pl.when(bits[level] == 1)
        def _():
            forward(level).wait_send()

    @pl.when(zhi == 0)
    def _():
        up.wait_send()

    @pl.when(zhi == 1)
    def _():
        slices(5).wait_send()
        forward(5).wait_send()

    seven = sqs_ref.at[pl.ds(0, GROUP - 1)]
    remote(seven, seven, sq_ss, sq_rs, partner).wait_recv()
    remote(seven, seven, sq_ss, sq_rs, partner).wait_send()

    whole = sqs_ref[0]
    for g in range(1, GROUP):
        whole = whole + sqs_ref[g]
    inv = lax.rsqrt(whole / CHANNELS + 1e-05)
    turned = jnp.concatenate([inv, jnp.zeros((CH - 8, CH), F32)], axis=0).T
    for c in range(NC):
        out_ref[c] = (y_ref[c] * turned[:, c:c + 1]).astype(BF16)


def shards(queries, keys, values, log_decay, level_weight, skip, norm_gain):
    hbm = pl.BlockSpec(memory_space=pltpu.HBM)
    dma = pltpu.SemaphoreType.DMA

    def stay(x):
        return pltpu.with_memory_space_constraint(x, pltpu.HBM)

    out = pl.pallas_call(
        kernel,
        out_shape=jax.ShapeDtypeStruct((NC, CH, ROWS), BF16),
        in_specs=[hbm] * 7,
        out_specs=pl.BlockSpec(memory_space=pltpu.VMEM),
        scratch_shapes=[
            pltpu.VMEM((NC, CH, STATE), BF16),
            pltpu.VMEM((NC, CH, STATE), BF16),
            pltpu.VMEM((NC, CH, ROWS), BF16),
            pltpu.VMEM((HEADS, TOK), F32),
            pltpu.VMEM((LEVELS + 1, HEADS, TOK), BF16),
            pltpu.SMEM((HEADS,), F32),
            pltpu.VMEM((ROWS,), BF16),
            dma((6 + NC,)),
            pltpu.VMEM((NC, HEADS, CH), F32),
            pltpu.VMEM((NC, CH, CH), F32),
            pltpu.VMEM((NC, HEADS, CH), F32),
            pltpu.VMEM((NC, HEADS, CH), F32),
            pltpu.VMEM((NC, HEADS, CH), F32),
            pltpu.VMEM((LEVELS, NC, HEADS, CH), F32),
            pltpu.VMEM((NC, ROWS, CH), BF16),
            pltpu.VMEM((NC, ROWS, STATE), BF16),
            pltpu.VMEM((ROWS, STATE), F32),
            pltpu.VMEM((NC, ROWS, CH), F32),
            pltpu.VMEM((NC, CH, ROWS), F32),
            pltpu.VMEM((HEADS + 8, CH), F32),
            pltpu.VMEM((HEADS + 8, CH), F32),
            pltpu.VMEM((HEADS, CH), F32),
            pltpu.VMEM((HALF, STATE), F32),
            pltpu.VMEM((1, CH), F32),
            pltpu.VMEM((CHIPS, 1, CH), F32),
            pltpu.VMEM((CHIPS, SLICE, STATE), F32),
            pltpu.VMEM((8, SLICE, STATE), F32),
            pltpu.VMEM((LEVELS, ROWS, STATE), F32),
            pltpu.VMEM((NC // 2, STATE, 2 * CH), BF16),
            pltpu.VMEM((HALF, STATE), BF16),
            pltpu.VMEM((8, CH), F32),
            pltpu.VMEM((GROUP, 8, CH), F32),
            dma, dma, dma, dma, dma, dma, dma, dma, dma, dma, dma, dma,
            dma((LEVELS,)), dma((LEVELS,)), dma, dma, dma((LEVELS,)), dma((LEVELS,)), dma, dma,
            pltpu.SemaphoreType.REGULAR, pltpu.SemaphoreType.REGULAR,
        ],
        compiler_params=pltpu.CompilerParams(
            collective_id=0, has_side_effects=True, vmem_limit_bytes=50 << 20),
        name="layer",
    )(
        stay(queries.reshape(NC, CH, STATE)), stay(keys.reshape(NC, CH, STATE)),
        stay(values.reshape(NC, CH, ROWS)), stay(log_decay), stay(level_weight), stay(skip),
        stay(norm_gain),
    )
    return out.reshape(TOK, ROWS)


def solution(mesh):
    placed = (
        P("seq", None), P("seq", None), P("seq", "head"), P("head", "seq"),
        P(None, "head", "seq"), P("head"), P("head"),
    )
    return jax.shard_map(
        shards, mesh=mesh, in_specs=placed, out_specs=P("seq", "head"), check_vma=False
    )
```

```python
import jax
import jax.numpy as jnp
from jax import lax
from jax.experimental import pallas as pl
from jax.experimental.pallas import tpu as pltpu
from jax.sharding import PartitionSpec as P

F32 = jnp.float32
BF16 = jnp.bfloat16
NT = (((1,), (1,)), ((), ()))

TOK = 768
CH = 128
NC = TOK // CH
HEADS = 16
HH = HEADS // 2
DIM = 64
STATE = 128
ROWS = HEADS * DIM
HALF = ROWS // 2
PLANE = 32
CHIPS = 16
SLICE = HALF // CHIPS
LEVELS = 6
GROUP = 8
CHANNELS = 8192
STARTS = {2: 0, 3: 4, 4: 6, 5: 7}
SIDE = 4
STEPS = sorted(
    ((dx, dy) for dx in range(SIDE) for dy in range(SIDE) if dx + dy > 0),
    key=lambda d: -min(d[0], SIDE - d[0]) - min(d[1], SIDE - d[1]))


def rows_of(start, size):
    return pl.ds(pl.multiple_of(start, SLICE), size)


def kernel(
    q_hbm, k_hbm, v_hbm, ld_hbm, lw_hbm, skip_hbm, gain_hbm, out_ref,
    q_ref, k_ref, v_ref, ld_ref, lw_ref, skip_ref, gain_ref, in_sem,
    lc_ref, lct_ref, w0_ref, ci_ref, cum_ref, coef_ref, vt_ref, sc_ref, rb_ref, run_ref, st_ref, acc_ref, y_ref,
    comb_ref, pcomb_ref, fall_ref, pair_ref, crow_ref, crows_ref,
    gath_ref, node_ref, bucket_ref, qt_ref, bb_ref, sq_ref, sqs_ref,
    ex_ss, ex_rs, cb_ss, cb_rs, l0_ss, l0_rs, cr_ss, cr_rs, p1_ss, p1_rs, n1_ss, n1_rs,
    p2_ss, p2_rs, z_ss, z_rs, fw_ss, fw_rs, sq_ss, sq_rs, here_z, here_h,
):
    seq = lax.axis_index("seq")
    head = lax.axis_index("head")
    zhi = seq // PLANE
    me = seq % PLANE
    chip = me // 2
    core = me % 2
    base = zhi * PLANE
    bits = [core] + [(chip // (1 << b)) % 2 for b in range(4)] + [zhi]

    def at(s):
        return {"seq": s, "head": head}

    cx = chip % SIDE
    cy = chip // SIDE

    def away(step):
        return SIDE * ((cy + step[1]) % SIDE) + (cx + step[0]) % SIDE

    def same_core(to):
        return at(base + 2 * to + core)

    def remote(src, dst, ss, rs, device):
        return pltpu.make_async_remote_copy(
            src_ref=src, dst_ref=dst, send_sem=ss, recv_sem=rs,
            device_id=device, device_id_type=pl.DeviceIdType.MESH,
        )

    partner = at(base + me + 1 - 2 * core)
    zpeer = at(seq + PLANE - 2 * PLANE * zhi)
    half = rows_of(HALF * core, HALF)
    other = rows_of(HALF * (1 - core), HALF)
    mine = HALF * core + SLICE * chip

    pairs = [(ld_hbm, ld_ref), (k_hbm, k_ref), (lw_hbm, lw_ref), (q_hbm, q_ref),
             (skip_hbm, skip_ref), (gain_hbm, gain_ref)]
    loads = [pltpu.make_async_copy(src, dst, in_sem.at[i]) for i, (src, dst) in enumerate(pairs)]
    loads[0].start()
    for c in range(NC):
        pltpu.make_async_copy(v_hbm.at[c], v_ref.at[c], in_sem.at[6 + c]).start()
    for copy in loads[1:]:
        copy.start()

    barrier = pltpu.get_barrier_semaphore()

    def greet(device, sem=barrier):
        pl.semaphore_signal(sem, inc=1, device_id=device, device_id_type=pl.DeviceIdType.MESH)

    def rank_of(h):
        return h + zhi * (GROUP - 1 - 2 * h)

    def peer(r):
        return (head + r) % GROUP

    rank = rank_of(head)

    for step in STEPS:
        greet(same_core(away(step)))

    greet(partner)

    @pl.when(zhi == 0)
    def _():
        greet(zpeer)

    @pl.loop(1, GROUP)
    def _(r):
        @pl.when(rank_of(peer(r)) > rank)
        def _():
            greet({"seq": seq, "head": peer(r)})

    loads[0].wait()
    row = lax.broadcasted_iota(jnp.int32, (CH, CH), 0)
    col = lax.broadcasted_iota(jnp.int32, (CH, CH), 1)
    tri = jnp.where(row <= col, 1.0, 0.0).astype(BF16)
    his, mids, los = [], [], []
    for c in range(NC):
        x = ld_ref[:, c * CH:(c + 1) * CH]
        hi = x.astype(BF16)
        rest = x - hi.astype(F32)
        mid = rest.astype(BF16)
        his.append(hi)
        mids.append(mid)
        los.append((rest - mid.astype(F32)).astype(BF16))
    sums = jnp.dot(jnp.concatenate(his + mids + los, axis=0), tri, preferred_element_type=F32)
    n = HEADS * NC
    total = jnp.zeros((HEADS, CH), F32)
    trow = jnp.zeros((1, CH), F32)
    for c in range(NC):
        a = HEADS * c
        lc = sums[a:a + HEADS] + sums[n + a:n + a + HEADS] + sums[2 * n + a:2 * n + a + HEADS]
        lc_ref[c] = lc
        cum_ref[c] = lc + total
        turned = jnp.concatenate([lc, jnp.zeros((CH - HEADS, CH), F32)], axis=0).T
        lct_ref[c] = turned
        trow = trow + turned[CH - 1:CH]
        total = total + jnp.broadcast_to(lc[:, CH - 1:CH], (HEADS, CH))
    comb_ref[0:HEADS] = total
    comb_ref[HEADS:HEADS + 8] = jnp.broadcast_to(trow, (8, CH))

    loads[1].wait()

    @pl.loop(0, NC)
    def _(c):
        pltpu.make_async_copy(v_hbm.at[c], v_ref.at[c], in_sem.at[6 + c]).wait()
        tail = jnp.exp(comb_ref[0:HEADS] - cum_ref[c])
        for j in range(ROWS // CH):
            vt = v_ref[c, :, j * CH:(j + 1) * CH].T
            vt_ref[c, j * CH:(j + 1) * CH, :] = vt
            wide = vt.astype(F32)
            for i in range(2):
                h = 2 * j + i
                sc_ref[c, h * DIM:(h + 1) * DIM] = (
                    wide[i * DIM:(i + 1) * DIM] * tail[h:h + 1]).astype(BF16)

    st_ref[...] = jnp.dot(
        jnp.concatenate([sc_ref[c] for c in range(NC)], axis=1),
        k_ref[...].reshape(TOK, STATE), preferred_element_type=F32)

    pl.semaphore_wait(barrier, CHIPS - 1 + 1 + rank + zhi)

    swap = remote(st_ref.at[other], bucket_ref.at[0, other], ex_ss, ex_rs, partner)
    comb = remote(comb_ref, pcomb_ref, cb_ss, cb_rs, partner)
    zero = remote(st_ref.at[half], bucket_ref.at[0, half], l0_ss, l0_rs, partner)
    swap.start()
    comb.start()

    @pl.when(zhi == 1)
    def _():
        greet(zpeer, here_z)

    @pl.loop(1, GROUP)
    def _(r):
        @pl.when(rank_of(peer(r)) < rank)
        def _():
            greet({"seq": seq, "head": peer(r)}, here_h)

    loads[2].wait()
    for copy in loads[3:]:
        copy.wait()
    for c in range(NC):
        w0 = lw_ref[0, :, c * CH:(c + 1) * CH].astype(F32)
        w0_ref[c] = w0
        ci_ref[c] = w0 * jnp.exp(lc_ref[c])
        qt_ref[c // 2, :, (c % 2) * CH:(c % 2 + 1) * CH] = q_ref[c].T

    def inside(first, last):
        @pl.loop(first, last)
        def _(c):
            qc = q_ref[c]
            s = lax.dot_general(k_ref[c], qc, NT, preferred_element_type=F32)
            r0 = lax.broadcasted_iota(jnp.int32, (CH, CH), 0)
            c0 = lax.broadcasted_iota(jnp.int32, (CH, CH), 1)
            s = jnp.where(r0 <= c0, s, 0.0)
            inter = lax.dot_general(rb_ref[c], qc, NT, preferred_element_type=F32)
            for h in range(HEADS):
                rows = slice(h * DIM, (h + 1) * DIM)
                d = jnp.minimum(lc_ref[c, h:h + 1] - lct_ref[c, :, h:h + 1], 0.0)
                mix = (jnp.exp(d) * s).astype(BF16)
                vt = vt_ref[c, rows]
                o = jnp.dot(vt, mix, preferred_element_type=F32)
                acc_ref[c, rows] = (
                    w0_ref[c, h:h + 1] * o + ci_ref[c, h:h + 1] * inter[rows]
                    + skip_ref[h] * vt.astype(F32))

    rb_ref[0] = jnp.zeros((ROWS, STATE), BF16)
    run_ref[...] = jnp.zeros((ROWS, STATE), F32)

    def prefix(first, last):
        @pl.loop(first, last)
        def _(c):
            lc = lc_ref[c]
            end = jnp.broadcast_to(lc[:, CH - 1:CH], (HEADS, CH))
            fall = jnp.exp(end)
            tail = jnp.exp(end - lc)
            scaled = [
                (vt_ref[c, h * DIM:(h + 1) * DIM].astype(F32) * tail[h:h + 1]).astype(BF16)
                for h in range(HEADS)]
            new = jnp.dot(jnp.concatenate(scaled, axis=0), k_ref[c], preferred_element_type=F32)
            for h in range(HEADS):
                rows = slice(h * DIM, (h + 1) * DIM)
                state = fall[h:h + 1] * run_ref[rows] + new[rows]
                run_ref[rows] = state
                rb_ref[c + 1, rows] = state.astype(BF16)

    prefix(0, 3)

    comb.wait_recv()
    remote(st_ref.at[half], bucket_ref.at[0, half], ex_ss, ex_rs, partner).wait_recv()
    late = jnp.where(core == 0, pcomb_ref[0:HEADS], comb_ref[0:HEADS])
    fall_ref[...] = jnp.exp(late)
    for i in range(HH):
        at_head = rows_of(HALF * core + DIM * i, DIM)
        own, got = st_ref[at_head], bucket_ref[0, at_head]
        left = jnp.where(core == 0, own, got)
        right = jnp.where(core == 0, got, own)
        pair_ref[i * DIM:(i + 1) * DIM] = fall_ref[pl.ds(HH * core + i, 1), :] * left + right
    crow = comb_ref[HEADS:HEADS + 1] + pcomb_ref[HEADS:HEADS + 1]
    crow_ref[...] = crow
    crows_ref[chip] = crow

    for step in STEPS:
        to = away(step)
        remote(pair_ref.at[rows_of(SLICE * to, SLICE)], gath_ref.at[chip], p1_ss, p1_rs,
               same_core(to)).start()
        remote(crow_ref, crows_ref.at[chip], cr_ss, cr_rs, same_core(to)).start()

    @pl.when(core == 0)
    def _():
        zero.start()

    first_level = remote(
        pair_ref, bucket_ref.at[1, half], n1_ss, n1_rs, same_core(chip + 1 - 2 * bits[1]))

    gath_ref[chip] = pair_ref[rows_of(SLICE * chip, SLICE)]

    prefix(3, NC - 1)
    inside(0, 3)

    @pl.when(bits[1] == 0)
    def _():
        first_level.start()

    inside(3, NC)

    fifteen = pl.ds(0, CHIPS - 1)
    crs = remote(crows_ref.at[fifteen], crows_ref.at[fifteen], cr_ss, cr_rs, partner)
    p1s = remote(gath_ref.at[fifteen], gath_ref.at[fifteen], p1_ss, p1_rs, partner)
    crs.wait_recv()
    p1s.wait_recv()

    lane = lax.broadcasted_iota(jnp.int32, (1, CH), 1)
    pick = lane == HH * core + chip // 2
    nodes = [gath_ref[i] for i in range(CHIPS)]
    weights = [
        jnp.sum(jnp.where(pick, crows_ref[i], 0.0), axis=1, keepdims=True) for i in range(CHIPS)]
    slot = 0
    for level in range(2, LEVELS):
        count = len(nodes) // 2
        joined = [
            jnp.exp(jnp.broadcast_to(weights[2 * j + 1], (1, CH))) * nodes[2 * j] + nodes[2 * j + 1]
            for j in range(count)
        ]
        weights = [weights[2 * j] + weights[2 * j + 1] for j in range(count)]
        nodes = joined
        for j in range(0, count, 2):
            node_ref[slot] = nodes[j]
            slot += 1

    up = remote(
        node_ref.at[STARTS[5]], bucket_ref.at[5, rows_of(mine, SLICE)], z_ss, z_rs, zpeer)

    for level in range(2, 5):
        for step in STEPS:
            to = away(step)

            @pl.when((to // (1 << (level - 1))) % 2 == 1)
            def _():
                remote(
                    node_ref.at[STARTS[level] + to // (1 << level)],
                    bucket_ref.at[level, rows_of(mine, SLICE)],
                    p2_ss.at[level], p2_rs.at[level], same_core(to)).start()

    @pl.when(zhi == 0)
    def _():
        pl.semaphore_wait(here_z, 1)
        up.start()

    for level in range(2, 5):
        @pl.when(bits[level] == 1)
        def _():
            bucket_ref[level, rows_of(mine, SLICE)] = node_ref[STARTS[level] + chip // (1 << level)]

    before = [jnp.zeros((1, CH), F32) for _ in range(LEVELS)]
    for i in range(CHIPS - 1):
        t = crows_ref[i]
        for level in range(2, LEVELS):
            counts = (i < chip) & (i >= chip - chip % (1 << (level - 1)))
            before[level] = before[level] + jnp.where(counts, t, 0.0)
    turned = jnp.concatenate(before + [jnp.zeros((CH - LEVELS, CH), F32)], axis=0).T
    inner = jnp.where(core == 1, pcomb_ref[0:HEADS], 0.0)
    for level in range(LEVELS):
        off = jnp.zeros((HEADS, CH), F32)
        if level > 0:
            off = inner
        if level > 1:
            off = off + jnp.broadcast_to(turned[0:HEADS, level:level + 1], (HEADS, CH))
        for c in range(NC):
            w = lw_ref[level + 1, :, c * CH:(c + 1) * CH].astype(F32)
            coef_ref[level, c] = w * jnp.exp(cum_ref[c] + off)

    def cross(level, side):
        at_half = rows_of(HALF * side, HALF)
        bb_ref[...] = bucket_ref[level, at_half].astype(BF16)

        for d in range(NC // 2):
            o = jnp.dot(bb_ref[...], qt_ref[d], preferred_element_type=F32)
            for i in range(2):
                c = 2 * d + i
                for h in range(HH):
                    rows = rows_of(HALF * side + DIM * h, DIM)
                    acc_ref[c, rows] = (
                        acc_ref[c, rows]
                        + coef_ref[level, c, pl.ds(HH * side + h, 1), :]
                        * o[h * DIM:(h + 1) * DIM, i * CH:(i + 1) * CH])

    def forward(level):
        return remote(
            bucket_ref.at[level, half], bucket_ref.at[level, half],
            fw_ss.at[level], fw_rs.at[level], partner)

    def forwarded(level):
        return remote(
            bucket_ref.at[level, other], bucket_ref.at[level, other],
            fw_ss.at[level], fw_rs.at[level], partner)

    some = pl.ds(0, (CHIPS - 1) * SLICE)

    def slices(level):
        part = bucket_ref.at[level, some]
        return remote(part, part, p2_ss.at[level], p2_rs.at[level], partner)

    @pl.when(core == 1)
    def _():
        cross(0, 1)
        remote(st_ref.at[other], bucket_ref.at[0, other], l0_ss, l0_rs, partner).wait_recv()
        cross(0, 0)

    @pl.when(zhi == 1)
    def _():
        up.wait_recv()
        own = bucket_ref.at[5, rows_of(mine, SLICE)]

        for step in STEPS:
            remote(own, own, p2_ss.at[5], p2_rs.at[5], same_core(away(step))).start()

    @pl.when(bits[1] == 1)
    def _():
        first_level.wait_recv()
        forward(1).start()
        cross(1, core)
        forwarded(1).wait_recv()
        cross(1, 1 - core)

    def landed(level):
        slices(level).wait_recv()
        forward(level).start()

    def rest(level):
        forwarded(level).wait_recv()
        cross(level, 1 - core)

    @pl.when(bits[2] == 1)
    def _():
        landed(2)
        cross(2, core)

    @pl.when((bits[2] == 1) & (core == 0))
    def _():
        rest(2)

    for level in range(3, 5):
        @pl.when(bits[level] == 1)
        def _():
            landed(level)

    for level in range(3, 5):
        @pl.when(bits[level] == 1)
        def _():
            cross(level, core)

    @pl.when((bits[2] == 1) & (core == 1))
    def _():
        rest(2)

    @pl.when(zhi == 1)
    def _():
        landed(5)
        cross(5, core)

    sq_ref[...] = jnp.zeros((8, CH), F32)

    def squares(c, rows):
        y = acc_ref[c, rows]
        return jnp.sum(y * y, axis=0, keepdims=True)

    for c in range(NC):
        sq_ref[c:c + 1] = squares(c, half)

    for level in range(3, LEVELS):
        @pl.when(bits[level] == 1)
        def _():
            rest(level)

    for c in range(NC):
        sq_ref[c:c + 1] = sq_ref[c:c + 1] + squares(c, other)
    sqs_ref[head] = sq_ref[...]

    @pl.when(rank < GROUP - 1)
    def _():
        pl.semaphore_wait(here_h, GROUP - 1 - rank)

    @pl.loop(1, GROUP)
    def _(r):
        remote(
            sq_ref, sqs_ref.at[head], sq_ss, sq_rs,
            {"seq": seq, "head": (head + r) % GROUP}).start()

    gain = gain_ref[...].reshape(1, ROWS).astype(F32)

    @pl.loop(0, NC)
    def _(c):
        for j in range(ROWS // CH):
            cols = slice(j * CH, (j + 1) * CH)
            y_ref[c, :, cols] = acc_ref[c, cols].T * gain[:, cols]

    swap.wait_send()
    comb.wait_send()
    crs.wait_send()
    p1s.wait_send()

    @pl.when(core == 0)
    def _():
        zero.wait_send()

    @pl.when(bits[1] == 0)
    def _():
        first_level.wait_send()

    @pl.when(bits[1] == 1)
    def _():
        forward(1).wait_send()

    for level in range(2, 5):
        for has in range(2):
            @pl.when(bits[level] == has)
            def _():
                sent = bucket_ref.at[level, pl.ds(0, (CHIPS // 2 - has) * SLICE)]
                remote(sent, sent, p2_ss.at[level], p2_rs.at[level], partner).wait_send()

        @pl.when(bits[level] == 1)
        def _():
            forward(level).wait_send()

    @pl.when(zhi == 0)
    def _():
        up.wait_send()

    @pl.when(zhi == 1)
    def _():
        slices(5).wait_send()
        forward(5).wait_send()

    seven = sqs_ref.at[pl.ds(0, GROUP - 1)]
    remote(seven, seven, sq_ss, sq_rs, partner).wait_recv()
    remote(seven, seven, sq_ss, sq_rs, partner).wait_send()

    whole = sqs_ref[0]
    for g in range(1, GROUP):
        whole = whole + sqs_ref[g]
    inv = lax.rsqrt(whole / CHANNELS + 1e-05)
    turned = jnp.concatenate([inv, jnp.zeros((CH - 8, CH), F32)], axis=0).T
    for c in range(NC):
        out_ref[c] = (y_ref[c] * turned[:, c:c + 1]).astype(BF16)


def shards(queries, keys, values, log_decay, level_weight, skip, norm_gain):
    hbm = pl.BlockSpec(memory_space=pltpu.HBM)
    dma = pltpu.SemaphoreType.DMA

    def stay(x):
        return pltpu.with_memory_space_constraint(x, pltpu.HBM)

    out = pl.pallas_call(
        kernel,
        out_shape=jax.ShapeDtypeStruct((NC, CH, ROWS), BF16),
        in_specs=[hbm] * 7,
        out_specs=pl.BlockSpec(memory_space=pltpu.VMEM),
        scratch_shapes=[
            pltpu.VMEM((NC, CH, STATE), BF16),
            pltpu.VMEM((NC, CH, STATE), BF16),
            pltpu.VMEM((NC, CH, ROWS), BF16),
            pltpu.VMEM((HEADS, TOK), F32),
            pltpu.VMEM((LEVELS + 1, HEADS, TOK), BF16),
            pltpu.SMEM((HEADS,), F32),
            pltpu.VMEM((ROWS,), BF16),
            dma((6 + NC,)),
            pltpu.VMEM((NC, HEADS, CH), F32),
            pltpu.VMEM((NC, CH, CH), F32),
            pltpu.VMEM((NC, HEADS, CH), F32),
            pltpu.VMEM((NC, HEADS, CH), F32),
            pltpu.VMEM((NC, HEADS, CH), F32),
            pltpu.VMEM((LEVELS, NC, HEADS, CH), F32),
            pltpu.VMEM((NC, ROWS, CH), BF16),
            pltpu.VMEM((NC, ROWS, CH), BF16),
            pltpu.VMEM((NC, ROWS, STATE), BF16),
            pltpu.VMEM((ROWS, STATE), F32),
            pltpu.VMEM((ROWS, STATE), F32),
            pltpu.VMEM((NC, ROWS, CH), F32),
            pltpu.VMEM((NC, CH, ROWS), F32),
            pltpu.VMEM((HEADS + 8, CH), F32),
            pltpu.VMEM((HEADS + 8, CH), F32),
            pltpu.VMEM((HEADS, CH), F32),
            pltpu.VMEM((HALF, STATE), F32),
            pltpu.VMEM((1, CH), F32),
            pltpu.VMEM((CHIPS, 1, CH), F32),
            pltpu.VMEM((CHIPS, SLICE, STATE), F32),
            pltpu.VMEM((8, SLICE, STATE), F32),
            pltpu.VMEM((LEVELS, ROWS, STATE), F32),
            pltpu.VMEM((NC // 2, STATE, 2 * CH), BF16),
            pltpu.VMEM((HALF, STATE), BF16),
            pltpu.VMEM((8, CH), F32),
            pltpu.VMEM((GROUP, 8, CH), F32),
            dma, dma, dma, dma, dma, dma, dma, dma, dma, dma, dma, dma,
            dma((LEVELS,)), dma((LEVELS,)), dma, dma, dma((LEVELS,)), dma((LEVELS,)), dma, dma,
            pltpu.SemaphoreType.REGULAR, pltpu.SemaphoreType.REGULAR,
        ],
        compiler_params=pltpu.CompilerParams(
            collective_id=0, has_side_effects=True, vmem_limit_bytes=50 << 20),
        name="layer",
    )(
        stay(queries.reshape(NC, CH, STATE)), stay(keys.reshape(NC, CH, STATE)),
        stay(values.reshape(NC, CH, ROWS)), stay(log_decay), stay(level_weight), stay(skip),
        stay(norm_gain),
    )
    return out.reshape(TOK, ROWS)


def solution(mesh):
    placed = (
        P("seq", None), P("seq", None), P("seq", "head"), P("head", "seq"),
        P(None, "head", "seq"), P("head"), P("head"),
    )
    return jax.shard_map(
        shards, mesh=mesh, in_specs=placed, out_specs=P("seq", "head"), check_vma=False
    )
```
